32 devices in a mesh: row: 8 (over z, y), col: 4 (over x, core).
Axes of the slice: x: 2, y: 2, z: 4, core: 2. Of those that a mesh axis runs over, the one named last changes fastest.
Arguments:
- q_start: bfloat16 [8192, 32], P(('row', 'col')), may hold values from -6 to 6
- row_scale: float32 [8192], P(('row', 'col')), may hold values from 0.25 to 4
- near_blocks: bfloat16 [8, 128, 256, 256], P('row', 'col'), may hold values from -0.0625 to 0.0625
- near_rows: int32 [8, 4, 32], P('row', 'col'), may hold values from 0 to 3
- near_cols: int32 [8, 4, 32], P('row', 'col'), may hold values from 0 to 7
- far_ut: bfloat16 [8, 512, 32, 256], P('row', 'col'), may hold values from -0.1875 to 0.1875
- far_vt: bfloat16 [8, 512, 32, 256], P('row', 'col'), may hold values from -0.375 to 0.375
- far_rank: int32 [8, 4, 128], P('row', 'col'), may hold values from 8 to 32, as said below
- far_rows: int32 [8, 4, 128], P('row', 'col'), may hold values from 0 to 3
- far_cols: int32 [8, 4, 128], P('row', 'col'), may hold values from 0 to 7
Outputs:
- basis: float32 [8192, 32], P(('row', 'col'))
- factor: float32 [32, 32], replicated
The draws below stay inside these ranges and needn't reach their ends.
Inputs may be any that keep to these rules, and one draw needn't show every extreme that they name: `far_rank`: each device has a far block of rank 32.
All inputs are finite; a program needn't handle non-finite values.
Results may differ from the reference program's by a relative error of at most 0.016.
Values may be sent and summed in bfloat16 or wider, within the bound.
A program may use at most 128 MiB of HBM per device.

```python
import math
import jax
import jax.numpy as jnp
from jax import lax

LEAF = 256
KCOLS = 32
RANK = 32
ROWS_DEV = 256
NEAR_DEV = 32
FAR_DEV = 128
ITERS = 4
NPTS = 8192
RCL = 4
CCL = 8
N_ROW = 8
N_COL = 4


def draw_far_rank(key, part):
    ranks = jax.random.randint(key, (N_ROW, N_COL, FAR_DEV), RANK // 4, RANK + 1)
    return ranks.at[:, :, 0].set(RANK).astype(jnp.int32)


def touch_ends(array, stream_key, smallest, high):
    longest = array.shape.index(max(array.shape))
    spots = []
    for shift in (0, 1):
        where = [jax.random.randint(jax.random.fold_in(stream_key, axis), (), 0, length) for axis, length in enumerate(array.shape)]
        where[longest] = (where[longest] + shift) % array.shape[longest]
        spots.append(tuple(where))
    return array.at[spots[0]].set(smallest).at[spots[1]].set(high)


def level_of(rng, extent, pieces, low, largest):
    def one(position, shards_of):
        steps = jax.random.uniform(jax.random.fold_in(jax.random.fold_in(rng, 6), position), (shards_of,), jnp.float32, low / len(pieces), largest / len(pieces))
        return jnp.repeat(jnp.exp(steps), extent[position] // shards_of).reshape((-1,) + (1,) * (len(extent) - position - 1))

    gain = one(*pieces[0])
    for cut in pieces[1:]:
        gain = gain * one(*cut)
    return gain


def bell_draw(key, dims, spread, limit, cuts=(), kind=jnp.bfloat16):
    result = jax.random.normal(key, dims, jnp.float32) * spread
    if len(cuts) > 0:
        result = level_of(key, dims, cuts, -0.22, 0.18) * result
    return jnp.clip(result, min=-limit, max=limit).astype(kind)


def setup_inputs(seed: int = 0) -> dict:
    keys = jax.random.split(jax.random.key(seed), 11)
    return {
        "q_start": bell_draw(keys[0], (NPTS, KCOLS), 1.0, 6.0, ((0, 32),)),
        "row_scale": jnp.clip(jnp.exp(math.log(4.0) - 2.7725887 * jax.random.uniform(keys[1], (NPTS,), jnp.float32) ** level_of(keys[1], (NPTS,), ((0, 32),), -0.2, 0.2)), 0.25, 4.0),
        "near_blocks": bell_draw(keys[2], (N_ROW, N_COL * NEAR_DEV, LEAF, LEAF), (LEAF * NEAR_DEV) ** -0.5, 0.0625, ((0, 8), (1, 4))),
        "near_rows": touch_ends(jax.random.randint(keys[3], (N_ROW, N_COL, NEAR_DEV), 0, RCL), jax.random.fold_in(keys[3], 1), 0, RCL - 1).astype(jnp.int32),
        "near_cols": touch_ends(jax.random.randint(keys[4], (N_ROW, N_COL, NEAR_DEV), 0, CCL), jax.random.fold_in(keys[4], 1), 0, CCL - 1).astype(jnp.int32),
        "far_ut": bell_draw(keys[5], (N_ROW, N_COL * FAR_DEV, RANK, LEAF), (RANK * FAR_DEV // 4) ** -0.5, 0.1875, ((0, 8), (1, 4))),
        "far_vt": bell_draw(keys[6], (N_ROW, N_COL * FAR_DEV, RANK, LEAF), LEAF ** -0.5, 0.375, ((0, 8), (1, 4))),
        "far_rank": draw_far_rank(jax.random.fold_in(keys[10], 71), 0),
        "far_rows": touch_ends(jax.random.randint(keys[8], (N_ROW, N_COL, FAR_DEV), 0, RCL), jax.random.fold_in(keys[8], 1), 0, RCL - 1).astype(jnp.int32),
        "far_cols": touch_ends(jax.random.randint(keys[9], (N_ROW, N_COL, FAR_DEV), 0, CCL), jax.random.fold_in(keys[9], 1), 0, CCL - 1).astype(jnp.int32),
    }


def block_apply(q_col, blocks, n_rows, n_cols, ut, vt, ranks, f_rows, f_cols):
    picked = q_col[n_cols].astype(jnp.float32)
    near_part = jnp.einsum('bij,bjk->bik', blocks.astype(jnp.float32), picked)
    clusters = jnp.arange(RCL, dtype=jnp.int32)
    near_hot = (clusters[:, None] == n_rows[None, :]).astype(jnp.float32)
    total = jnp.dot(near_hot, near_part.reshape(near_part.shape[0], LEAF * KCOLS), precision=lax.Precision.HIGHEST)
    far_q = q_col[f_cols].astype(jnp.float32)
    inner = jnp.einsum('brl,blk->brk', vt.astype(jnp.float32), far_q)
    keep = jnp.arange(RANK, dtype=jnp.int32)[None, :] < ranks[:, None]
    inner = jnp.where(keep[:, :, None], inner, 0.0).astype(jnp.bfloat16)
    far_part = jnp.einsum('brl,brk->blk', ut.astype(jnp.float32), inner.astype(jnp.float32))
    far_hot = (clusters[:, None] == f_rows[None, :]).astype(jnp.float32)
    total = total + jnp.dot(far_hot, far_part.reshape(far_part.shape[0], LEAF * KCOLS), precision=lax.Precision.HIGHEST)
    return total

def reference(q_start, row_scale, near_blocks, near_rows, near_cols, far_ut, far_vt, far_rank, far_rows, far_cols):
    basis_bf = q_start
    basis = q_start.astype(jnp.float32)
    factor = jnp.zeros((KCOLS, KCOLS), jnp.float32)
    for step in range(ITERS):
        q_cols = basis_bf.reshape(N_ROW, N_COL, ROWS_DEV, KCOLS).transpose(1, 0, 2, 3).reshape(N_COL, CCL, LEAF, KCOLS)

        def one_row(items):
            blocks, n_rows, n_cols, ut, vt, ranks, f_rows, f_cols = items
            blocks = blocks.reshape(N_COL, NEAR_DEV, LEAF, LEAF)
            ut = ut.reshape(N_COL, FAR_DEV, RANK, LEAF)
            vt = vt.reshape(N_COL, FAR_DEV, RANK, LEAF)

            def add_col(carry, xs):
                return (carry + block_apply(*xs), None)
            start = jnp.zeros((RCL, LEAF * KCOLS), jnp.float32)
            total, unused = lax.scan(add_col, start, (q_cols, blocks, n_rows, n_cols, ut, vt, ranks, f_rows, f_cols))
            return total
        rows_all = lax.map(one_row, (near_blocks, near_rows, near_cols, far_ut, far_vt, far_rank, far_rows, far_cols))
        product = rows_all.reshape(RCL * N_ROW, LEAF, KCOLS).reshape(NPTS, KCOLS) * row_scale[:, None]
        gram = jnp.dot(product.T, product, precision=lax.Precision.HIGHEST) / NPTS
        factor = jnp.linalg.cholesky(gram)
        basis = lax.linalg.triangular_solve(factor, product, left_side=False, lower=True, transpose_a=True)
        basis_bf = basis.astype(jnp.bfloat16)
    return (basis, factor)
```

```python
import functools

import jax
import jax.numpy as jnp
from jax import lax
from jax.experimental import pallas as pl
from jax.experimental.pallas import tpu as pltpu
from jax.sharding import PartitionSpec as P

ITERS = 4
MESH = pl.DeviceIdType.MESH
HIGH = lax.Precision.HIGHEST
NT = (((1,), (1,)), ((), ()))
LANES = 128
SUB = 8
TILE = 256


def dot_nt(a, b, precision=None):
    return lax.dot_general(a, b, NT, precision=precision, preferred_element_type=jnp.float32)


def partner(index, step, size):
    if size & (size - 1):
        return lax.rem(index + step, size)
    out, bit = 0, 1
    while bit < size:
        mine = (index // bit) % 2
        out = out + bit * (1 - mine if step & bit else mine)
        bit *= 2
    return out


def factorize(work, kcols):
    blocks = kcols // SUB
    w = [work[SUB * q : SUB * (q + 1), :] for q in range(blocks)]
    sub = lax.broadcasted_iota(jnp.int32, (SUB, LANES), 0)
    diag = []
    for p in range(blocks):
        cb = [
            [
                jnp.broadcast_to(w[q][:, kcols + SUB * p + j : kcols + SUB * p + j + 1], (SUB, LANES))
                if q >= p
                else None
                for q in range(blocks)
            ]
            for j in range(SUB)
        ]
        dp = jnp.ones((SUB, LANES), jnp.float32)
        for j in range(SUB):
            d = jnp.broadcast_to(cb[j][p][j : j + 1, :], (SUB, LANES))
            dp = jnp.where(sub == j, d, dp)
            inv = 1.0 / d
            row = jnp.broadcast_to(w[p][j : j + 1, :], (SUB, LANES)) * inv
            others = {
                k: jnp.broadcast_to(cb[k][p][j : j + 1, :], (SUB, LANES)) * inv
                for k in range(j + 1, SUB)
            }
            for q in range(p, blocks):
                m = cb[j][q]
                if q == p:
                    m = jnp.where(sub > j, m, 0.0)
                w[q] = w[q] - m * row
                for k in range(j + 1, SUB):
                    cb[k][q] = cb[k][q] - m * others[k]
        diag.append(dp)
    return jnp.concatenate([w[q] * lax.rsqrt(diag[q]) for q in range(blocks)], axis=0)


def apply_inverse(rows, product):
    pad = jnp.zeros((LANES - product.shape[0], product.shape[1]), jnp.float32)
    return jnp.dot(
        rows,
        jnp.concatenate([product, pad], axis=0),
        precision=HIGH,
        preferred_element_type=jnp.float32,
    )


def finish(rows_ref, prod_ref, basis_ref, factor_ref):
    rows = rows_ref[...]
    kcols = rows.shape[0]
    lane = lax.broadcasted_iota(jnp.int32, rows.shape, 1)
    sub = lax.broadcasted_iota(jnp.int32, rows.shape, 0)
    basis_ref[...] = apply_inverse(rows, prod_ref[...])
    upper = jnp.where(lane - kcols >= sub, rows, 0.0)
    pick = jnp.where(lane == sub + kcols, 1.0, 0.0).astype(jnp.float32)
    factor_ref[...] = dot_nt(pick, upper, HIGH)


def kernel(
    n_row,
    n_col,
    total_pts,
    q_hbm,
    scale_hbm,
    rank_hbm,
    fr_hbm,
    fc_hbm,
    nr_hbm,
    nc_hbm,
    near_hbm,
    ut_hbm,
    vt_hbm,
    rows_ref,
    prod_ref,
    scale_ref,
    rank_ref,
    fr_ref,
    fc_ref,
    nr_ref,
    nc_ref,
    near_ref,
    ut_ref,
    vt_ref,
    ag_refs,
    sel_ref,
    lhs_ref,
    part_ref,
    out_ref,
    rs_ref,
    ga_ref,
    gb_ref,
    load_sem,
    ag_send,
    ag_recv,
    rs_send,
    rs_recv,
    ga_send,
    ga_recv,
    gb_send,
    gb_recv,
):
    row = lax.axis_index("row")
    col = lax.axis_index("col")
    kcols, leaf = q_hbm.shape
    groups = LANES // kcols
    far_tiles = ut_ref.shape[0] // TILE
    n_near = near_ref.shape[0]
    rank_max = ut_ref.shape[0] // rank_ref.shape[0]

    pair = 2 if n_row % 2 == 0 else 1
    low, high = lax.rem(row, pair), row // pair
    n_low, n_high = n_col * pair, n_row // pair
    peers = [(partner(row, d, n_row), col) for d in range(1, n_row)]
    for e in range(pair):
        for d in range(1, n_col):
            peers.append((high * pair + lax.rem(low + e, pair), lax.rem(col + d, n_col)))
    barrier = pltpu.get_barrier_semaphore()
    for peer in peers:
        pl.semaphore_signal(barrier, inc=1, device_id=peer, device_id_type=MESH)

    moves = (
        (q_hbm, ag_refs[0].at[row]),
        (rank_hbm, rank_ref),
        (fr_hbm, fr_ref),
        (fc_hbm, fc_ref),
        (vt_hbm, vt_ref),
        (ut_hbm, ut_ref),
        (nr_hbm, nr_ref),
        (nc_hbm, nc_ref),
        (scale_hbm, scale_ref),
        (near_hbm, near_ref),
    )
    loads = [
        pltpu.make_async_copy(src, dst, load_sem.at[i]) for i, (src, dst) in enumerate(moves)
    ]
    for copy in loads:
        copy.start()

    def ag_copy(t, peer):
        return pltpu.make_async_remote_copy(
            src_ref=ag_refs[t].at[row],
            dst_ref=ag_refs[t].at[row],
            send_sem=ag_send.at[t],
            recv_sem=ag_recv.at[t],
            device_id=(peer, col),
            device_id_type=MESH,
        )

    def gather_start(t):
        for d in range(n_row - 1, 0, -1):
            ag_copy(t, partner(row, d, n_row)).start()

    def wait_like(view, sem):
        pltpu.make_async_copy(view, view, sem).wait()

    def gather_wait(t):
        view = ag_refs[t].at[pl.ds(0, n_row - 1)]
        wait_like(view, ag_send.at[t])
        wait_like(view, ag_recv.at[t])

    def scatter_start(t):
        for d in range(n_col - 1, 0, -1):
            peer = lax.rem(col + d, n_col)
            pltpu.make_async_remote_copy(
                src_ref=out_ref.at[t, peer],
                dst_ref=rs_ref.at[t, d - 1],
                send_sem=rs_send.at[t],
                recv_sem=rs_recv.at[t],
                device_id=(row, peer),
                device_id_type=MESH,
            ).start()

    def scatter_wait(t):
        view = rs_ref.at[t]
        wait_like(view, rs_send.at[t])
        wait_like(view, rs_recv.at[t])

    def gram_low_start(t, value):
        mine = low * n_col + col
        ga_ref[t, mine] = value
        for e in range(pair - 1, -1, -1):
            for d in range(n_col - 1, -1, -1):
                if (d, e) == (0, 0):
                    continue
                pltpu.make_async_remote_copy(
                    src_ref=ga_ref.at[t, mine],
                    dst_ref=ga_ref.at[t, mine],
                    send_sem=ga_send.at[t],
                    recv_sem=ga_recv.at[t],
                    device_id=(
                        high * pair + lax.rem(low + e, pair),
                        lax.rem(col + d, n_col),
                    ),
                    device_id_type=MESH,
                ).start()

    def gram_high_start(t):
        view = ga_ref.at[t, pl.ds(0, n_low - 1)]
        wait_like(view, ga_send.at[t])
        wait_like(view, ga_recv.at[t])
        gb_ref[t, high] = jnp.sum(ga_ref[t], axis=0)
        for d in range(n_high - 1, 0, -1):
            pltpu.make_async_remote_copy(
                src_ref=gb_ref.at[t, high],
                dst_ref=gb_ref.at[t, high],
                send_sem=gb_send.at[t],
                recv_sem=gb_recv.at[t],
                device_id=(partner(high, d, n_high) * pair + low, col),
                device_id_type=MESH,
            ).start()

    def gram_wait(t):
        view = gb_ref.at[t, pl.ds(0, n_high - 1)]
        wait_like(view, gb_send.at[t])
        wait_like(view, gb_recv.at[t])

    def selectors():
        place = lax.broadcasted_iota(jnp.int32, (SUB, TILE), 1)
        owner, rank_of = place // rank_max, lax.rem(place, rank_max)

        def tile(i, carry):
            fc = jnp.zeros((SUB, TILE), jnp.int32)
            fr, keep = fc, fc
            for j in range(TILE // rank_max):
                b = i * (TILE // rank_max) + j
                fc = jnp.where(owner == j, fc_ref[b], fc)
                fr = jnp.where(owner == j, fr_ref[b], fr)
                keep = jnp.where(owner == j, rank_ref[b], keep)
            start = pl.multiple_of(i * TILE, TILE)
            sel_ref[0, :, pl.ds(start, TILE)] = jnp.where(rank_of < keep, fc, -1)
            sel_ref[1, :, pl.ds(start, TILE)] = fr
            return carry

        lax.fori_loop(0, far_tiles, tile, 0)

    def operator(t, first):
        if first:
            loads[4].wait()
        q_all = ag_refs[t][...].reshape(n_row * kcols, leaf)

        def far_tile(i, carry):
            start = pl.multiple_of(i * TILE, TILE)
            y = dot_nt(q_all, vt_ref[pl.ds(start, TILE), :])
            fc = jnp.concatenate([sel_ref[0, :, pl.ds(start, TILE)]] * (kcols // SUB), axis=0)
            fr = jnp.concatenate([sel_ref[1, :, pl.ds(start, TILE)]] * (kcols // SUB), axis=0)
            inner = jnp.zeros((kcols, TILE), jnp.float32)
            for c in range(n_row):
                inner = jnp.where(fc == c, y[c * kcols : (c + 1) * kcols, :], inner)
            for r in range(n_col):
                lhs_ref[r * kcols : (r + 1) * kcols, pl.ds(start, TILE)] = jnp.where(
                    fr == r, inner, 0.0
                ).astype(jnp.bfloat16)
            return carry

        lax.fori_loop(0, far_tiles, far_tile, 0, unroll=True)
        if first:
            loads[5].wait()
        far = jnp.dot(lhs_ref[...], ut_ref[...], preferred_element_type=jnp.float32)
        for r in range(n_col):
            part_ref[t, r] = far[r * kcols : (r + 1) * kcols, :]
        if first:
            for i in (6, 7, 9):
                loads[i].wait()

        def near_block(b, acc):
            z = dot_nt(ag_refs[t][nc_ref[b]], near_ref[b])
            r_of = nr_ref[b]
            return tuple(
                a + z * jnp.where(r_of == r, 1.0, 0.0).astype(jnp.float32) for r, a in enumerate(acc)
            )

        zero = jnp.zeros((kcols, leaf), jnp.float32)
        near = lax.fori_loop(0, n_near, near_block, (zero,) * n_col, unroll=True)
        for r in range(n_col):
            whole = part_ref[t, r] + near[r]
            part_ref[t, r] = whole
            out_ref[t, r] = whole.astype(jnp.bfloat16)

    lane = lax.broadcasted_iota(jnp.int32, (SUB, LANES), 1)
    lane_full = lax.broadcasted_iota(jnp.int32, (kcols, LANES), 1)
    sub_full = lax.broadcasted_iota(jnp.int32, (kcols, LANES), 0)

    def pack_gram(product):
        tiled = jnp.concatenate([product] * groups, axis=0)
        g = dot_nt(product, tiled, HIGH)
        rows = kcols // groups
        packed = jnp.zeros((rows, LANES), jnp.float32)
        for i in range(groups):
            packed = jnp.where(lane // kcols == i, g[i * rows : (i + 1) * rows, :], packed)
        return packed

    def solve(t):
        g = jnp.sum(gb_ref[t], axis=0) / total_pts
        parts = []
        for i in range(groups):
            shift = (1 - i) * kcols % LANES
            parts.append(pltpu.roll(g, shift, 1) if shift else g)
        s = jnp.concatenate(parts, axis=0)
        work = jnp.where(lane_full < kcols, jnp.where(lane_full == sub_full, 1.0, 0.0), s)
        work = jnp.where(lane_full < 2 * kcols, work, 0.0)
        return factorize(work, kcols)

    for i in (1, 2, 3):
        loads[i].wait()
    selectors()
    loads[0].wait()
    pl.semaphore_wait(barrier, len(peers))
    gather_start(0)
    for t in range(ITERS):
        if t > 0:
            gram_high_start(t - 1)
        gather_wait(t)
        operator(t, t == 0)
        scatter_start(t)
        if t > 0:
            gram_wait(t - 1)
            rows = solve(t - 1)
        if t == 0:
            loads[8].wait()
        scatter_wait(t)
        total = part_ref[t, col]
        for d in range(1, n_col):
            total = total + rs_ref[t, d - 1].astype(jnp.float32)
        product = total * scale_ref[...]
        if t > 0:
            product = apply_inverse(rows, product)
        if t < ITERS - 1:
            ag_refs[t + 1][row] = product.astype(jnp.bfloat16)
            gather_start(t + 1)
        gram_low_start(t, pack_gram(product))
    prod_ref[...] = product
    gram_high_start(ITERS - 1)
    gram_wait(ITERS - 1)
    rows_ref[...] = solve(ITERS - 1)


def on_device(
    q_start,
    row_scale,
    near_blocks,
    near_rows,
    near_cols,
    far_ut,
    far_vt,
    far_rank,
    far_rows,
    far_cols,
):
    leaf, kcols = q_start.shape
    n_row = lax.axis_size("row")
    n_col = lax.axis_size("col")
    n_dev = n_row * n_col
    pair = 2 if n_row % 2 == 0 else 1
    n_low, n_high = n_col * pair, n_row // pair
    n_near = near_blocks.shape[1]
    n_far, rank_max = far_ut.shape[1:3]
    near = near_blocks[0]
    ut = far_ut.reshape(n_far * rank_max, leaf)
    vt = far_vt.reshape(n_far * rank_max, leaf)
    vmem = pl.BlockSpec(memory_space=pltpu.VMEM)
    hbm = pl.BlockSpec(memory_space=pl.ANY)
    f32, bf16 = jnp.float32, jnp.bfloat16
    rows, product = pl.pallas_call(
        functools.partial(kernel, n_row, n_col, leaf * n_dev),
        name="subspace",
        out_shape=(
            pltpu.VMEM((kcols, LANES), f32),
            pltpu.VMEM((kcols, leaf), f32),
        ),
        in_specs=[hbm] * 10,
        out_specs=(vmem, vmem),
        scratch_shapes=[
            pltpu.VMEM((1, leaf), f32),
            pltpu.SMEM((n_far,), jnp.int32),
            pltpu.SMEM((n_far,), jnp.int32),
            pltpu.SMEM((n_far,), jnp.int32),
            pltpu.SMEM((n_near,), jnp.int32),
            pltpu.SMEM((n_near,), jnp.int32),
            pltpu.VMEM(near.shape, bf16),
            pltpu.VMEM(ut.shape, bf16),
            pltpu.VMEM(vt.shape, bf16),
            [pltpu.VMEM((n_row, kcols, leaf), bf16) for _ in range(ITERS)],
            pltpu.VMEM((2, SUB, n_far * rank_max), jnp.int32),
            pltpu.VMEM((n_col * kcols, n_far * rank_max), bf16),
            pltpu.VMEM((ITERS, n_col, kcols, leaf), f32),
            pltpu.VMEM((ITERS, n_col, kcols, leaf), bf16),
            pltpu.VMEM((ITERS, n_col - 1, kcols, leaf), bf16),
            pltpu.VMEM((ITERS, n_low, kcols * kcols // LANES, LANES), f32),
            pltpu.VMEM((ITERS, n_high, kcols * kcols // LANES, LANES), f32),
            pltpu.SemaphoreType.DMA((10,)),
            pltpu.SemaphoreType.DMA((ITERS,)),
            pltpu.SemaphoreType.DMA((ITERS,)),
            pltpu.SemaphoreType.DMA((ITERS,)),
            pltpu.SemaphoreType.DMA((ITERS,)),
            pltpu.SemaphoreType.DMA((ITERS,)),
            pltpu.SemaphoreType.DMA((ITERS,)),
            pltpu.SemaphoreType.DMA((ITERS,)),
            pltpu.SemaphoreType.DMA((ITERS,)),
        ],
        compiler_params=pltpu.CompilerParams(
            collective_id=0, has_side_effects=True, vmem_limit_bytes=56 * 1024 * 1024
        ),
    )(
        q_start.T,
        row_scale.reshape(1, leaf),
        far_rank[0, 0],
        far_rows[0, 0],
        far_cols[0, 0],
        near_rows[0, 0],
        near_cols[0, 0],
        near,
        ut,
        vt,
    )
    basis_t, factor = pl.pallas_call(
        finish,
        name="finish",
        out_shape=(
            jax.ShapeDtypeStruct((kcols, leaf), f32),
            jax.ShapeDtypeStruct((kcols, kcols), f32),
        ),
        in_specs=[vmem, vmem],
        out_specs=(vmem, vmem),
    )(*(pltpu.with_memory_space_constraint(x, pltpu.VMEM) for x in (rows, product)))
    return basis_t.T, factor


def solution(mesh):
    in_specs = (
        P(("row", "col"), None),
        P(("row", "col")),
        P("row", "col", None, None),
        P("row", "col", None),
        P("row", "col", None),
        P("row", "col", None, None),
        P("row", "col", None, None),
        P("row", "col", None),
        P("row", "col", None),
        P("row", "col", None),
    )
    out_specs = (P(("row", "col"), None), P())
    return jax.shard_map(
        on_device, mesh=mesh, in_specs=in_specs, out_specs=out_specs, check_vma=False
    )
```

```python
import functools

import jax
import jax.numpy as jnp
from jax import lax
from jax.experimental import pallas as pl
from jax.experimental.pallas import tpu as pltpu
from jax.sharding import PartitionSpec as P

ITERS = 4
MESH = pl.DeviceIdType.MESH
HIGH = lax.Precision.HIGHEST
NT = (((1,), (1,)), ((), ()))
LANES = 128
SUB = 8
TILE = 256


def dot_nt(a, b, precision=None):
    return lax.dot_general(a, b, NT, precision=precision, preferred_element_type=jnp.float32)


def partner(index, step, size):
    if size & (size - 1):
        return lax.rem(index + step, size)
    out, bit = 0, 1
    while bit < size:
        mine = (index // bit) % 2
        out = out + bit * (1 - mine if step & bit else mine)
        bit *= 2
    return out


def factorize(work, kcols):
    blocks = kcols // SUB
    w = [work[SUB * q : SUB * (q + 1), :] for q in range(blocks)]
    sub = lax.broadcasted_iota(jnp.int32, (SUB, LANES), 0)
    diag = []
    for p in range(blocks):
        cb = [
            [
                jnp.broadcast_to(w[q][:, kcols + SUB * p + j : kcols + SUB * p + j + 1], (SUB, LANES))
                if q >= p
                else None
                for q in range(blocks)
            ]
            for j in range(SUB)
        ]
        dp = jnp.ones((SUB, LANES), jnp.float32)
        for j in range(SUB):
            d = jnp.broadcast_to(cb[j][p][j : j + 1, :], (SUB, LANES))
            dp = jnp.where(sub == j, d, dp)
            inv = 1.0 / d
            row = jnp.broadcast_to(w[p][j : j + 1, :], (SUB, LANES)) * inv
            others = {
                k: jnp.broadcast_to(cb[k][p][j : j + 1, :], (SUB, LANES)) * inv
                for k in range(j + 1, SUB)
            }
            for q in range(p, blocks):
                m = cb[j][q]
                if q == p:
                    m = jnp.where(sub > j, m, 0.0)
                w[q] = w[q] - m * row
                for k in range(j + 1, SUB):
                    cb[k][q] = cb[k][q] - m * others[k]
        diag.append(dp)
    return jnp.concatenate([w[q] * lax.rsqrt(diag[q]) for q in range(blocks)], axis=0)


def apply_inverse(rows, product):
    pad = jnp.zeros((LANES - product.shape[0], product.shape[1]), jnp.float32)
    return jnp.dot(
        rows,
        jnp.concatenate([product, pad], axis=0),
        precision=HIGH,
        preferred_element_type=jnp.float32,
    )


def finish(rows_ref, prod_ref, basis_ref, factor_ref):
    rows = rows_ref[...]
    kcols = rows.shape[0]
    lane = lax.broadcasted_iota(jnp.int32, rows.shape, 1)
    sub = lax.broadcasted_iota(jnp.int32, rows.shape, 0)
    basis_ref[...] = apply_inverse(rows, prod_ref[...])
    upper = jnp.where(lane - kcols >= sub, rows, 0.0)
    pick = jnp.where(lane == sub + kcols, 1.0, 0.0).astype(jnp.float32)
    factor_ref[...] = dot_nt(pick, upper, HIGH)


def kernel(
    n_row,
    n_col,
    total_pts,
    q_hbm,
    scale_hbm,
    rank_hbm,
    fr_hbm,
    fc_hbm,
    nr_hbm,
    nc_hbm,
    near_hbm,
    ut_hbm,
    vt_hbm,
    rows_ref,
    prod_ref,
    scale_ref,
    rank_ref,
    fr_ref,
    fc_ref,
    nr_ref,
    nc_ref,
    near_ref,
    ut_ref,
    vt_ref,
    ag_refs,
    sel_ref,
    lhs_ref,
    part_ref,
    out_ref,
    rs_ref,
    ga_ref,
    gb_ref,
    gd_ref,
    load_sem,
    ag_send,
    ag_recv,
    rs_send,
    rs_recv,
    ga_send,
    ga_recv,
    gb_send,
    gb_recv,
    gd_sem,
):
    row = lax.axis_index("row")
    col = lax.axis_index("col")
    kcols, leaf = q_hbm.shape
    groups = LANES // kcols
    far_tiles = ut_ref.shape[0] // TILE
    n_near = near_ref.shape[0]
    rank_max = ut_ref.shape[0] // rank_ref.shape[0]

    pair = 2 if n_row % 2 == 0 else 1
    low, high = lax.rem(row, pair), row // pair
    n_low, n_high = n_col * pair, n_row // pair
    peers = [(partner(row, d, n_row), col) for d in range(1, n_row)]
    peers += [(row, partner(col, d, n_col)) for d in range(1, n_col)]
    barrier = pltpu.get_barrier_semaphore()
    for peer in peers:
        pl.semaphore_signal(barrier, inc=1, device_id=peer, device_id_type=MESH)

    moves = (
        (q_hbm, ag_refs[0].at[row]),
        (rank_hbm, rank_ref),
        (fr_hbm, fr_ref),
        (fc_hbm, fc_ref),
        (vt_hbm, vt_ref),
        (ut_hbm, ut_ref),
        (nr_hbm, nr_ref),
        (nc_hbm, nc_ref),
        (scale_hbm, scale_ref),
        (near_hbm, near_ref),
    )
    loads = [
        pltpu.make_async_copy(src, dst, load_sem.at[i]) for i, (src, dst) in enumerate(moves)
    ]
    for copy in loads:
        copy.start()

    def ag_copy(t, peer):
        return pltpu.make_async_remote_copy(
            src_ref=ag_refs[t].at[row],
            dst_ref=ag_refs[t].at[row],
            send_sem=ag_send.at[t],
            recv_sem=ag_recv.at[t],
            device_id=(peer, col),
            device_id_type=MESH,
        )

    def gather_start(t):
        for d in range(n_row - 1, 0, -1):
            ag_copy(t, partner(row, d, n_row)).start()

    def wait_like(view, sem):
        pltpu.make_async_copy(view, view, sem).wait()

    def gather_wait(t):
        view = ag_refs[t].at[pl.ds(0, n_row - 1)]
        wait_like(view, ag_send.at[t])
        wait_like(view, ag_recv.at[t])

    def scatter_start(t):
        for d in sorted(range(1, n_col), key=lambda d: (d % 2, -d)):
            peer = partner(col, d, n_col)
            pltpu.make_async_remote_copy(
                src_ref=out_ref.at[t, peer],
                dst_ref=rs_ref.at[t, d - 1],
                send_sem=rs_send.at[t],
                recv_sem=rs_recv.at[t],
                device_id=(row, peer),
                device_id_type=MESH,
            ).start()

    def scatter_wait(t):
        view = rs_ref.at[t]
        wait_like(view, rs_send.at[t])
        wait_like(view, rs_recv.at[t])

    def gram_low_start(t, value):
        mine = low * n_col + col
        ga_ref[t, mine] = value
        for e in range(pair - 1, -1, -1):
            for d in range(n_col - 1, -1, -1):
                if (d, e) == (0, 0):
                    continue
                pltpu.make_async_remote_copy(
                    src_ref=ga_ref.at[t, mine],
                    dst_ref=ga_ref.at[t, mine],
                    send_sem=ga_send.at[t],
                    recv_sem=ga_recv.at[t],
                    device_id=(
                        high * pair + lax.rem(low + e, pair),
                        lax.rem(col + d, n_col),
                    ),
                    device_id_type=MESH,
                ).start()

    def gram_high_start(t):
        view = ga_ref.at[t, pl.ds(0, n_low - 1)]
        wait_like(view, ga_send.at[t])
        wait_like(view, ga_recv.at[t])
        gb_ref[t, high] = jnp.sum(ga_ref[t], axis=0)
        for d in range(n_high - 1, 0, -1):
            pltpu.make_async_remote_copy(
                src_ref=gb_ref.at[t, high],
                dst_ref=gb_ref.at[t, high],
                send_sem=gb_send.at[t],
                recv_sem=gb_recv.at[t],
                device_id=(partner(high, d, n_high) * pair + low, col),
                device_id_type=MESH,
            ).start()

    def gram_all(value):
        mine = row * n_col + col
        gd_ref[mine] = value
        for e in range(n_row - 1, -1, -1):
            for d in range(n_col - 1, -1, -1):
                if (d, e) == (0, 0):
                    continue
                pltpu.make_async_remote_copy(
                    src_ref=gd_ref.at[mine],
                    dst_ref=gd_ref.at[mine],
                    send_sem=gd_sem.at[0],
                    recv_sem=gd_sem.at[1],
                    device_id=(partner(row, e, n_row), partner(col, d, n_col)),
                    device_id_type=MESH,
                ).start()
        view = gd_ref.at[pl.ds(0, n_row * n_col - 1)]
        wait_like(view, gd_sem.at[0])
        wait_like(view, gd_sem.at[1])
        return jnp.sum(gd_ref[...], axis=0)

    def gram_wait(t):
        view = gb_ref.at[t, pl.ds(0, n_high - 1)]
        wait_like(view, gb_send.at[t])
        wait_like(view, gb_recv.at[t])
        return jnp.sum(gb_ref[t], axis=0)

    def selectors():
        place = lax.broadcasted_iota(jnp.int32, (SUB, TILE), 1)
        owner, rank_of = place // rank_max, lax.rem(place, rank_max)

        def tile(i, carry):
            fc = jnp.zeros((SUB, TILE), jnp.int32)
            fr, keep = fc, fc
            for j in range(TILE // rank_max):
                b = i * (TILE // rank_max) + j
                fc = jnp.where(owner == j, fc_ref[b], fc)
                fr = jnp.where(owner == j, fr_ref[b], fr)
                keep = jnp.where(owner == j, rank_ref[b], keep)
            start = pl.multiple_of(i * TILE, TILE)
            sel_ref[0, :, pl.ds(start, TILE)] = jnp.where(rank_of < keep, fc, -1)
            sel_ref[1, :, pl.ds(start, TILE)] = fr
            return carry

        lax.fori_loop(0, far_tiles, tile, 0)

    def operator(t):
        q_all = ag_refs[t][...].reshape(n_row * kcols, leaf)

        def far_tile(i, carry):
            start = pl.multiple_of(i * TILE, TILE)
            y = dot_nt(q_all, vt_ref[pl.ds(start, TILE), :])
            fc = jnp.concatenate([sel_ref[0, :, pl.ds(start, TILE)]] * (kcols // SUB), axis=0)
            fr = jnp.concatenate([sel_ref[1, :, pl.ds(start, TILE)]] * (kcols // SUB), axis=0)
            inner = jnp.zeros((kcols, TILE), jnp.float32)
            for c in range(n_row):
                inner = jnp.where(fc == c, y[c * kcols : (c + 1) * kcols, :], inner)
            for r in range(n_col):
                lhs_ref[r * kcols : (r + 1) * kcols, pl.ds(start, TILE)] = jnp.where(
                    fr == r, inner, 0.0
                ).astype(jnp.bfloat16)
            return carry

        lax.fori_loop(0, far_tiles, far_tile, 0, unroll=True)
        far = jnp.dot(lhs_ref[...], ut_ref[...], preferred_element_type=jnp.float32)
        for r in range(n_col):
            part_ref[t, r] = far[r * kcols : (r + 1) * kcols, :]

        def near_block(b, acc):
            z = dot_nt(ag_refs[t][nc_ref[b]], near_ref[b])
            r_of = nr_ref[b]
            return tuple(
                a + z * jnp.where(r_of == r, 1.0, 0.0).astype(jnp.float32) for r, a in enumerate(acc)
            )

        zero = jnp.zeros((kcols, leaf), jnp.float32)
        near = lax.fori_loop(0, n_near, near_block, (zero,) * n_col, unroll=True)
        for r in range(n_col):
            whole = part_ref[t, r] + near[r]
            part_ref[t, r] = whole
            out_ref[t, r] = whole.astype(jnp.bfloat16)

    lane = lax.broadcasted_iota(jnp.int32, (SUB, LANES), 1)
    lane_full = lax.broadcasted_iota(jnp.int32, (kcols, LANES), 1)
    sub_full = lax.broadcasted_iota(jnp.int32, (kcols, LANES), 0)

    def pack_gram(product):
        tiled = jnp.concatenate([product] * groups, axis=0)
        g = dot_nt(product, tiled, HIGH)
        rows = kcols // groups
        packed = jnp.zeros((rows, LANES), jnp.float32)
        for i in range(groups):
            packed = jnp.where(lane // kcols == i, g[i * rows : (i + 1) * rows, :], packed)
        return packed

    def solve(g):
        g = g / total_pts
        parts = []
        for i in range(groups):
            shift = (1 - i) * kcols % LANES
            parts.append(pltpu.roll(g, shift, 1) if shift else g)
        s = jnp.concatenate(parts, axis=0)
        work = jnp.where(lane_full < kcols, jnp.where(lane_full == sub_full, 1.0, 0.0), s)
        work = jnp.where(lane_full < 2 * kcols, work, 0.0)
        return factorize(work, kcols)

    loads[0].wait()
    pl.semaphore_wait(barrier, len(peers))
    gather_start(0)
    for copy in loads[1:4]:
        copy.wait()
    selectors()
    for copy in loads[4:]:
        copy.wait()
    for t in range(ITERS):
        if t > 0:
            gram_high_start(t - 1)
        gather_wait(t)
        operator(t)
        scatter_start(t)
        if t > 0:
            rows = solve(gram_wait(t - 1))
        scatter_wait(t)
        total = part_ref[t, col]
        for d in range(1, n_col):
            total = total + rs_ref[t, d - 1].astype(jnp.float32)
        product = total * scale_ref[...]
        if t > 0:
            product = apply_inverse(rows, product)
        if t < ITERS - 1:
            ag_refs[t + 1][row] = product.astype(jnp.bfloat16)
            gather_start(t + 1)
            gram_low_start(t, pack_gram(product))
    prod_ref[...] = product
    rows_ref[...] = solve(gram_all(pack_gram(product)))


def on_device(
    q_start,
    row_scale,
    near_blocks,
    near_rows,
    near_cols,
    far_ut,
    far_vt,
    far_rank,
    far_rows,
    far_cols,
):
    leaf, kcols = q_start.shape
    n_row = lax.axis_size("row")
    n_col = lax.axis_size("col")
    n_dev = n_row * n_col
    pair = 2 if n_row % 2 == 0 else 1
    n_low, n_high = n_col * pair, n_row // pair
    n_near = near_blocks.shape[1]
    n_far, rank_max = far_ut.shape[1:3]
    near = near_blocks[0]
    ut = far_ut.reshape(n_far * rank_max, leaf)
    vt = far_vt.reshape(n_far * rank_max, leaf)
    vmem = pl.BlockSpec(memory_space=pltpu.VMEM)
    hbm = pl.BlockSpec(memory_space=pl.ANY)
    f32, bf16 = jnp.float32, jnp.bfloat16
    rows, product = pl.pallas_call(
        functools.partial(kernel, n_row, n_col, leaf * n_dev),
        name="subspace",
        out_shape=(
            pltpu.VMEM((kcols, LANES), f32),
            pltpu.VMEM((kcols, leaf), f32),
        ),
        in_specs=[hbm] * 10,
        out_specs=(vmem, vmem),
        scratch_shapes=[
            pltpu.VMEM((1, leaf), f32),
            pltpu.SMEM((n_far,), jnp.int32),
            pltpu.SMEM((n_far,), jnp.int32),
            pltpu.SMEM((n_far,), jnp.int32),
            pltpu.SMEM((n_near,), jnp.int32),
            pltpu.SMEM((n_near,), jnp.int32),
            pltpu.VMEM(near.shape, bf16),
            pltpu.VMEM(ut.shape, bf16),
            pltpu.VMEM(vt.shape, bf16),
            [pltpu.VMEM((n_row, kcols, leaf), bf16) for _ in range(ITERS)],
            pltpu.VMEM((2, SUB, n_far * rank_max), jnp.int32),
            pltpu.VMEM((n_col * kcols, n_far * rank_max), bf16),
            pltpu.VMEM((ITERS, n_col, kcols, leaf), f32),
            pltpu.VMEM((ITERS, n_col, kcols, leaf), bf16),
            pltpu.VMEM((ITERS, n_col - 1, kcols, leaf), bf16),
            pltpu.VMEM((ITERS - 1, n_low, kcols * kcols // LANES, LANES), f32),
            pltpu.VMEM((ITERS - 1, n_high, kcols * kcols // LANES, LANES), f32),
            pltpu.VMEM((n_dev, kcols * kcols // LANES, LANES), f32),
            pltpu.SemaphoreType.DMA((10,)),
            pltpu.SemaphoreType.DMA((ITERS,)),
            pltpu.SemaphoreType.DMA((ITERS,)),
            pltpu.SemaphoreType.DMA((ITERS,)),
            pltpu.SemaphoreType.DMA((ITERS,)),
            pltpu.SemaphoreType.DMA((ITERS,)),
            pltpu.SemaphoreType.DMA((ITERS,)),
            pltpu.SemaphoreType.DMA((ITERS,)),
            pltpu.SemaphoreType.DMA((ITERS,)),
            pltpu.SemaphoreType.DMA((2,)),
        ],
        compiler_params=pltpu.CompilerParams(
            collective_id=0, has_side_effects=True, vmem_limit_bytes=56 * 1024 * 1024
        ),
    )(
        q_start.T,
        row_scale.reshape(1, leaf),
        far_rank[0, 0],
        far_rows[0, 0],
        far_cols[0, 0],
        near_rows[0, 0],
        near_cols[0, 0],
        near,
        ut,
        vt,
    )
    basis_t, factor = pl.pallas_call(
        finish,
        name="finish",
        out_shape=(
            jax.ShapeDtypeStruct((kcols, leaf), f32),
            jax.ShapeDtypeStruct((kcols, kcols), f32),
        ),
        in_specs=[vmem, vmem],
        out_specs=(vmem, vmem),
    )(*(pltpu.with_memory_space_constraint(x, pltpu.VMEM) for x in (rows, product)))
    return basis_t.T, factor


def solution(mesh):
    in_specs = (
        P(("row", "col"), None),
        P(("row", "col")),
        P("row", "col", None, None),
        P("row", "col", None),
        P("row", "col", None),
        P("row", "col", None, None),
        P("row", "col", None, None),
        P("row", "col", None),
        P("row", "col", None),
        P("row", "col", None),
    )
    out_specs = (P(("row", "col"), None), P())
    return jax.shard_map(
        on_device, mesh=mesh, in_specs=in_specs, out_specs=out_specs, check_vma=False
    )
```

```python
import functools

import jax
import jax.numpy as jnp
from jax import lax
from jax.experimental import pallas as pl
from jax.experimental.pallas import tpu as pltpu
from jax.sharding import PartitionSpec as P

ITERS = 4
MESH = pl.DeviceIdType.MESH
HIGH = lax.Precision.HIGHEST
NT = (((1,), (1,)), ((), ()))
LANES = 128
SUB = 8
TILE = 256


def dot_nt(a, b, precision=None):
    return lax.dot_general(a, b, NT, precision=precision, preferred_element_type=jnp.float32)


def partner(index, step, size):
    if size & (size - 1):
        return lax.rem(index + step, size)
    out, bit = 0, 1
    while bit < size:
        mine = (index // bit) % 2
        out = out + bit * (1 - mine if step & bit else mine)
        bit *= 2
    return out


def factorize(work, kcols):
    blocks = kcols // SUB
    w = [work[SUB * q : SUB * (q + 1), :] for q in range(blocks)]
    sub = lax.broadcasted_iota(jnp.int32, (SUB, LANES), 0)
    diag = []
    for p in range(blocks):
        cb = [
            [
                jnp.broadcast_to(w[q][:, kcols + SUB * p + j : kcols + SUB * p + j + 1], (SUB, LANES))
                if q >= p
                else None
                for q in range(blocks)
            ]
            for j in range(SUB)
        ]
        dp = jnp.ones((SUB, LANES), jnp.float32)
        for j in range(SUB):
            d = jnp.broadcast_to(cb[j][p][j : j + 1, :], (SUB, LANES))
            dp = jnp.where(sub == j, d, dp)
            inv = 1.0 / d
            row = jnp.broadcast_to(w[p][j : j + 1, :], (SUB, LANES)) * inv
            others = {
                k: jnp.broadcast_to(cb[k][p][j : j + 1, :], (SUB, LANES)) * inv
                for k in range(j + 1, SUB)
            }
            for q in range(p, blocks):
                m = cb[j][q]
                if q == p:
                    m = jnp.where(sub > j, m, 0.0)
                w[q] = w[q] - m * row
                for k in range(j + 1, SUB):
                    cb[k][q] = cb[k][q] - m * others[k]
        diag.append(dp)
    return jnp.concatenate([w[q] * lax.rsqrt(diag[q]) for q in range(blocks)], axis=0)


def apply_inverse(rows, product):
    pad = jnp.zeros((LANES - product.shape[0], product.shape[1]), jnp.float32)
    return jnp.dot(
        rows,
        jnp.concatenate([product, pad], axis=0),
        precision=HIGH,
        preferred_element_type=jnp.float32,
    )


def finish(rows_ref, prod_ref, basis_ref, factor_ref):
    rows = rows_ref[...]
    kcols = rows.shape[0]
    lane = lax.broadcasted_iota(jnp.int32, rows.shape, 1)
    sub = lax.broadcasted_iota(jnp.int32, rows.shape, 0)
    basis_ref[...] = apply_inverse(rows, prod_ref[...])
    upper = jnp.where(lane - kcols >= sub, rows, 0.0)
    pick = jnp.where(lane == sub + kcols, 1.0, 0.0).astype(jnp.float32)
    factor_ref[...] = dot_nt(pick, upper, HIGH)


def kernel(
    n_row,
    n_col,
    total_pts,
    q_hbm,
    scale_hbm,
    rank_hbm,
    fr_hbm,
    fc_hbm,
    nr_hbm,
    nc_hbm,
    near_hbm,
    ut_hbm,
    vt_hbm,
    rows_ref,
    prod_ref,
    scale_ref,
    rank_ref,
    fr_ref,
    fc_ref,
    nr_ref,
    nc_ref,
    near_ref,
    ut_ref,
    vt_ref,
    ag_refs,
    sel_ref,
    lhs_ref,
    vt_t_ref,
    part_ref,
    out_ref,
    rs_ref,
    ga_ref,
    gb_ref,
    gd_ref,
    load_sem,
    ag_send,
    ag_recv,
    rs_send,
    rs_recv,
    ga_send,
    ga_recv,
    gb_send,
    gb_recv,
    gd_sem,
):
    row = lax.axis_index("row")
    col = lax.axis_index("col")
    kcols, leaf = q_hbm.shape
    groups = LANES // kcols
    far_tiles = ut_ref.shape[0] // TILE
    n_near = near_ref.shape[0]
    n_parts = 4 if n_near % 4 == 0 else 1
    rank_max = ut_ref.shape[0] // rank_ref.shape[0]

    pair = 2 if n_row % 2 == 0 else 1
    low, high = lax.rem(row, pair), row // pair
    n_low, n_high = n_col * pair, n_row // pair
    peers = [(partner(row, d, n_row), col) for d in range(1, n_row)]
    peers += [(row, partner(col, d, n_col)) for d in range(1, n_col)]
    barrier = pltpu.get_barrier_semaphore()
    for peer in peers:
        pl.semaphore_signal(barrier, inc=1, device_id=peer, device_id_type=MESH)

    size = n_near // n_parts
    parts = [pl.ds(i * size, size) for i in range(n_parts)]
    moves = (
        (q_hbm, ag_refs[0].at[row]),
        (rank_hbm, rank_ref),
        (fr_hbm, fr_ref),
        (fc_hbm, fc_ref),
        (nr_hbm, nr_ref),
        (nc_hbm, nc_ref),
        (scale_hbm, scale_ref),
        *((near_hbm.at[part], near_ref.at[part]) for part in parts),
        (vt_hbm, vt_ref),
        (ut_hbm, ut_ref),
    )
    loads = [
        pltpu.make_async_copy(src, dst, load_sem.at[i]) for i, (src, dst) in enumerate(moves)
    ]
    for copy in loads:
        copy.start()

    def ag_copy(t, peer):
        return pltpu.make_async_remote_copy(
            src_ref=ag_refs[t].at[row],
            dst_ref=ag_refs[t].at[row],
            send_sem=ag_send.at[t],
            recv_sem=ag_recv.at[t],
            device_id=(peer, col),
            device_id_type=MESH,
        )

    def gather_start(t):
        for d in range(n_row - 1, 0, -1):
            ag_copy(t, partner(row, d, n_row)).start()

    def wait_like(view, sem):
        pltpu.make_async_copy(view, view, sem).wait()

    def gather_wait(t):
        view = ag_refs[t].at[pl.ds(0, n_row - 1)]
        wait_like(view, ag_send.at[t])
        wait_like(view, ag_recv.at[t])

    def scatter_start(t):
        for d in sorted(range(1, n_col), key=lambda d: (d % 2, -d)):
            peer = partner(col, d, n_col)
            pltpu.make_async_remote_copy(
                src_ref=out_ref.at[t, peer],
                dst_ref=rs_ref.at[t, d - 1],
                send_sem=rs_send.at[t],
                recv_sem=rs_recv.at[t],
                device_id=(row, peer),
                device_id_type=MESH,
            ).start()

    def scatter_wait(t):
        view = rs_ref.at[t]
        wait_like(view, rs_send.at[t])
        wait_like(view, rs_recv.at[t])

    def gram_low_start(t, value):
        mine = low * n_col + col
        ga_ref[t, mine] = value
        for e in range(pair - 1, -1, -1):
            for d in range(n_col - 1, -1, -1):
                if (d, e) == (0, 0):
                    continue
                pltpu.make_async_remote_copy(
                    src_ref=ga_ref.at[t, mine],
                    dst_ref=ga_ref.at[t, mine],
                    send_sem=ga_send.at[t],
                    recv_sem=ga_recv.at[t],
                    device_id=(
                        high * pair + lax.rem(low + e, pair),
                        lax.rem(col + d, n_col),
                    ),
                    device_id_type=MESH,
                ).start()

    def gram_high_start(t):
        view = ga_ref.at[t, pl.ds(0, n_low - 1)]
        wait_like(view, ga_send.at[t])
        wait_like(view, ga_recv.at[t])
        gb_ref[t, high] = jnp.sum(ga_ref[t], axis=0)
        for d in range(n_high - 1, 0, -1):
            pltpu.make_async_remote_copy(
                src_ref=gb_ref.at[t, high],
                dst_ref=gb_ref.at[t, high],
                send_sem=gb_send.at[t],
                recv_sem=gb_recv.at[t],
                device_id=(partner(high, d, n_high) * pair + low, col),
                device_id_type=MESH,
            ).start()

    def gram_all(value):
        mine = row * n_col + col
        gd_ref[mine] = value
        for e in range(n_row - 1, -1, -1):
            for d in range(n_col - 1, -1, -1):
                if (d, e) == (0, 0):
                    continue
                pltpu.make_async_remote_copy(
                    src_ref=gd_ref.at[mine],
                    dst_ref=gd_ref.at[mine],
                    send_sem=gd_sem.at[0],
                    recv_sem=gd_sem.at[1],
                    device_id=(partner(row, e, n_row), partner(col, d, n_col)),
                    device_id_type=MESH,
                ).start()
        view = gd_ref.at[pl.ds(0, n_row * n_col - 1)]
        wait_like(view, gd_sem.at[0])
        wait_like(view, gd_sem.at[1])
        return jnp.sum(gd_ref[...], axis=0)

    def gram_wait(t):
        view = gb_ref.at[t, pl.ds(0, n_high - 1)]
        wait_like(view, gb_send.at[t])
        wait_like(view, gb_recv.at[t])
        return jnp.sum(gb_ref[t], axis=0)

    def selectors():
        place = lax.broadcasted_iota(jnp.int32, (SUB, TILE), 1)
        owner, rank_of = place // rank_max, lax.rem(place, rank_max)

        def tile(i, carry):
            fc = jnp.zeros((SUB, TILE), jnp.int32)
            fr, keep = fc, fc
            for j in range(TILE // rank_max):
                b = i * (TILE // rank_max) + j
                fc = jnp.where(owner == j, fc_ref[b], fc)
                fr = jnp.where(owner == j, fr_ref[b], fr)
                keep = jnp.where(owner == j, rank_ref[b], keep)
            start = pl.multiple_of(i * TILE, TILE)
            sel_ref[0, :, pl.ds(start, TILE)] = jnp.where(rank_of < keep, fc, -1)
            sel_ref[1, :, pl.ds(start, TILE)] = fr
            return carry

        lax.fori_loop(0, far_tiles, tile, 0)

    def operator(t):
        q_all = ag_refs[t][...].reshape(n_row * kcols, leaf)

        def far_tile(i):
            tile = slice(i * TILE, (i + 1) * TILE)
            y = jnp.dot(q_all, vt_t_ref[:, tile], preferred_element_type=jnp.float32)
            fc = jnp.concatenate([sel_ref[0, :, tile]] * (kcols // SUB), axis=0)
            fr = jnp.concatenate([sel_ref[1, :, tile]] * (kcols // SUB), axis=0)
            inner = jnp.zeros((kcols, TILE), jnp.float32)
            for c in range(n_row):
                inner = jnp.where(fc == c, y[c * kcols : (c + 1) * kcols, :], inner)
            for r in range(n_col):
                lhs_ref[r * kcols : (r + 1) * kcols, tile] = jnp.where(
                    fr == r, inner, 0.0
                ).astype(jnp.bfloat16)

        def near_block(b, acc):
            z = jnp.dot(ag_refs[t][nc_ref[b]], near_ref[b], preferred_element_type=jnp.float32)
            r_of = nr_ref[b]
            return [
                a + z * jnp.where(r_of == r, 1.0, 0.0).astype(jnp.float32)
                for r, a in enumerate(acc)
            ]

        near = [jnp.zeros((kcols, leaf), jnp.float32)] * n_col
        for i in range(far_tiles):
            far_tile(i)
            for b in range(i * n_near // far_tiles, (i + 1) * n_near // far_tiles):
                near = near_block(b, near)
        far = jnp.dot(lhs_ref[...], ut_ref[...], preferred_element_type=jnp.float32)
        for r in range(n_col):
            whole = near[r] + far[r * kcols : (r + 1) * kcols, :]
            part_ref[t, r] = whole
            out_ref[t, r] = whole.astype(jnp.bfloat16)

    lane = lax.broadcasted_iota(jnp.int32, (SUB, LANES), 1)
    lane_full = lax.broadcasted_iota(jnp.int32, (kcols, LANES), 1)
    sub_full = lax.broadcasted_iota(jnp.int32, (kcols, LANES), 0)

    def pack_gram(product):
        tiled = jnp.concatenate([product] * groups, axis=0)
        g = dot_nt(product, tiled, HIGH)
        rows = kcols // groups
        packed = jnp.zeros((rows, LANES), jnp.float32)
        for i in range(groups):
            packed = jnp.where(lane // kcols == i, g[i * rows : (i + 1) * rows, :], packed)
        return packed

    def solve(g):
        g = g / total_pts
        parts = []
        for i in range(groups):
            shift = (1 - i) * kcols % LANES
            parts.append(pltpu.roll(g, shift, 1) if shift else g)
        s = jnp.concatenate(parts, axis=0)
        work = jnp.where(lane_full < kcols, jnp.where(lane_full == sub_full, 1.0, 0.0), s)
        work = jnp.where(lane_full < 2 * kcols, work, 0.0)
        return factorize(work, kcols)

    loads[0].wait()
    pl.semaphore_wait(barrier, len(peers))
    gather_start(0)
    for copy in loads[1:4]:
        copy.wait()
    selectors()
    for i in range(n_parts):
        loads[7 + i].wait()
        for b in range(i * size, (i + 1) * size):
            near_ref[b] = near_ref[b].T
    loads[7 + n_parts].wait()
    for i in range(far_tiles):
        tile = slice(i * TILE, (i + 1) * TILE)
        vt_t_ref[:, tile] = vt_ref[tile, :].T
    for copy in (*loads[4:7], loads[8 + n_parts]):
        copy.wait()
    for t in range(ITERS):
        if t > 0:
            gram_high_start(t - 1)
        gather_wait(t)
        operator(t)
        scatter_start(t)
        if t > 0:
            rows = solve(gram_wait(t - 1))
        scatter_wait(t)
        total = part_ref[t, col]
        for d in range(1, n_col):
            total = total + rs_ref[t, d - 1].astype(jnp.float32)
        product = total * scale_ref[...]
        if t > 0:
            product = apply_inverse(rows, product)
        if t < ITERS - 1:
            ag_refs[t + 1][row] = product.astype(jnp.bfloat16)
            gather_start(t + 1)
            gram_low_start(t, pack_gram(product))
    prod_ref[...] = product
    rows_ref[...] = solve(gram_all(pack_gram(product)))


def on_device(
    q_start,
    row_scale,
    near_blocks,
    near_rows,
    near_cols,
    far_ut,
    far_vt,
    far_rank,
    far_rows,
    far_cols,
):
    leaf, kcols = q_start.shape
    n_row = lax.axis_size("row")
    n_col = lax.axis_size("col")
    n_dev = n_row * n_col
    pair = 2 if n_row % 2 == 0 else 1
    n_low, n_high = n_col * pair, n_row // pair
    n_near = near_blocks.shape[1]
    n_far, rank_max = far_ut.shape[1:3]
    near = near_blocks[0]
    ut = far_ut.reshape(n_far * rank_max, leaf)
    vt = far_vt.reshape(n_far * rank_max, leaf)
    vmem = pl.BlockSpec(memory_space=pltpu.VMEM)
    hbm = pl.BlockSpec(memory_space=pl.ANY)
    f32, bf16 = jnp.float32, jnp.bfloat16
    rows, product = pl.pallas_call(
        functools.partial(kernel, n_row, n_col, leaf * n_dev),
        name="subspace",
        out_shape=(
            pltpu.VMEM((kcols, LANES), f32),
            pltpu.VMEM((kcols, leaf), f32),
        ),
        in_specs=[hbm] * 10,
        out_specs=(vmem, vmem),
        scratch_shapes=[
            pltpu.VMEM((1, leaf), f32),
            pltpu.SMEM((n_far,), jnp.int32),
            pltpu.SMEM((n_far,), jnp.int32),
            pltpu.SMEM((n_far,), jnp.int32),
            pltpu.SMEM((n_near,), jnp.int32),
            pltpu.SMEM((n_near,), jnp.int32),
            pltpu.VMEM(near.shape, bf16),
            pltpu.VMEM(ut.shape, bf16),
            pltpu.VMEM(vt.shape, bf16),
            [pltpu.VMEM((n_row, kcols, leaf), bf16) for _ in range(ITERS)],
            pltpu.VMEM((2, SUB, n_far * rank_max), jnp.int32),
            pltpu.VMEM((n_col * kcols, n_far * rank_max), bf16),
            pltpu.VMEM((leaf, n_far * rank_max), bf16),
            pltpu.VMEM((ITERS, n_col, kcols, leaf), f32),
            pltpu.VMEM((ITERS, n_col, kcols, leaf), bf16),
            pltpu.VMEM((ITERS, n_col - 1, kcols, leaf), bf16),
            pltpu.VMEM((ITERS - 1, n_low, kcols * kcols // LANES, LANES), f32),
            pltpu.VMEM((ITERS - 1, n_high, kcols * kcols // LANES, LANES), f32),
            pltpu.VMEM((n_dev, kcols * kcols // LANES, LANES), f32),
            pltpu.SemaphoreType.DMA((13,)),
            pltpu.SemaphoreType.DMA((ITERS,)),
            pltpu.SemaphoreType.DMA((ITERS,)),
            pltpu.SemaphoreType.DMA((ITERS,)),
            pltpu.SemaphoreType.DMA((ITERS,)),
            pltpu.SemaphoreType.DMA((ITERS,)),
            pltpu.SemaphoreType.DMA((ITERS,)),
            pltpu.SemaphoreType.DMA((ITERS,)),
            pltpu.SemaphoreType.DMA((ITERS,)),
            pltpu.SemaphoreType.DMA((2,)),
        ],
        compiler_params=pltpu.CompilerParams(
            collective_id=0, has_side_effects=True, vmem_limit_bytes=56 * 1024 * 1024
        ),
    )(
        q_start.T,
        row_scale.reshape(1, leaf),
        far_rank[0, 0],
        far_rows[0, 0],
        far_cols[0, 0],
        near_rows[0, 0],
        near_cols[0, 0],
        near,
        ut,
        vt,
    )
    basis_t, factor = pl.pallas_call(
        finish,
        name="finish",
        out_shape=(
            jax.ShapeDtypeStruct((kcols, leaf), f32),
            jax.ShapeDtypeStruct((kcols, kcols), f32),
        ),
        in_specs=[vmem, vmem],
        out_specs=(vmem, vmem),
    )(*(pltpu.with_memory_space_constraint(x, pltpu.VMEM) for x in (rows, product)))
    return basis_t.T, factor


def solution(mesh):
    in_specs = (
        P(("row", "col"), None),
        P(("row", "col")),
        P("row", "col", None, None),
        P("row", "col", None),
        P("row", "col", None),
        P("row", "col", None, None),
        P("row", "col", None, None),
        P("row", "col", None),
        P("row", "col", None),
        P("row", "col", None),
    )
    out_specs = (P(("row", "col"), None), P())
    return jax.shard_map(
        on_device, mesh=mesh, in_specs=in_specs, out_specs=out_specs, check_vma=False
    )
```

```python
import functools

import jax
import jax.numpy as jnp
from jax import lax
from jax.experimental import pallas as pl
from jax.experimental.pallas import tpu as pltpu
from jax.sharding import PartitionSpec as P

ITERS = 4
MESH = pl.DeviceIdType.MESH
HIGH = lax.Precision.HIGHEST
NT = (((1,), (1,)), ((), ()))
LANES = 128
SUB = 8
TILE = 256


def dot_nt(a, b, precision=None):
    return lax.dot_general(a, b, NT, precision=precision, preferred_element_type=jnp.float32)


def partner(index, step, size):
    if size & (size - 1):
        return lax.rem(index + step, size)
    out, bit = 0, 1
    while bit < size:
        mine = (index // bit) % 2
        out = out + bit * (1 - mine if step & bit else mine)
        bit *= 2
    return out


def factorize(work, kcols):
    blocks = kcols // SUB
    w = [work[SUB * q : SUB * (q + 1), :] for q in range(blocks)]
    sub = lax.broadcasted_iota(jnp.int32, (SUB, LANES), 0)
    diag = []
    for p in range(blocks):
        cb = [
            [
                jnp.broadcast_to(w[q][:, kcols + SUB * p + j : kcols + SUB * p + j + 1], (SUB, LANES))
                if q >= p
                else None
                for q in range(blocks)
            ]
            for j in range(SUB)
        ]
        dp = jnp.ones((SUB, LANES), jnp.float32)
        for j in range(SUB):
            d = jnp.broadcast_to(cb[j][p][j : j + 1, :], (SUB, LANES))
            dp = jnp.where(sub == j, d, dp)
            inv = 1.0 / d
            row = jnp.broadcast_to(w[p][j : j + 1, :], (SUB, LANES)) * inv
            others = {
                k: jnp.broadcast_to(cb[k][p][j : j + 1, :], (SUB, LANES)) * inv
                for k in range(j + 1, SUB)
            }
            for q in range(p, blocks):
                m = cb[j][q]
                if q == p:
                    m = jnp.where(sub > j, m, 0.0)
                w[q] = w[q] - m * row
                for k in range(j + 1, SUB):
                    cb[k][q] = cb[k][q] - m * others[k]
        diag.append(dp)
    return jnp.concatenate([w[q] * lax.rsqrt(diag[q]) for q in range(blocks)], axis=0)


def apply_inverse(rows, product):
    pad = jnp.zeros((LANES - product.shape[0], product.shape[1]), jnp.float32)
    return jnp.dot(
        rows,
        jnp.concatenate([product, pad], axis=0),
        precision=HIGH,
        preferred_element_type=jnp.float32,
    )


def finish(rows_ref, prod_ref, basis_ref, factor_ref):
    rows = rows_ref[...]
    kcols = rows.shape[0]
    lane = lax.broadcasted_iota(jnp.int32, rows.shape, 1)
    sub = lax.broadcasted_iota(jnp.int32, rows.shape, 0)
    basis_ref[...] = apply_inverse(rows, prod_ref[...])
    upper = jnp.where(lane - kcols >= sub, rows, 0.0)
    pick = jnp.where(lane == sub + kcols, 1.0, 0.0).astype(jnp.float32)
    factor_ref[...] = dot_nt(pick, upper, HIGH)


def kernel(
    n_row,
    n_col,
    total_pts,
    q_hbm,
    scale_hbm,
    rank_hbm,
    fr_hbm,
    fc_hbm,
    nr_hbm,
    nc_hbm,
    near_hbm,
    ut_hbm,
    vt_hbm,
    rows_ref,
    prod_ref,
    scale_ref,
    rank_ref,
    fr_ref,
    fc_ref,
    nr_ref,
    nc_ref,
    near_ref,
    ut_ref,
    vt_ref,
    ag_refs,
    sel_ref,
    inner_ref,
    lhs_ref,
    vt_t_ref,
    part_ref,
    out_ref,
    rs_ref,
    ga_ref,
    gb_ref,
    gd_ref,
    load_sem,
    ag_send,
    ag_recv,
    rs_send,
    rs_recv,
    ga_send,
    ga_recv,
    gb_send,
    gb_recv,
    gd_sem,
):
    row = lax.axis_index("row")
    col = lax.axis_index("col")
    kcols, leaf = q_hbm.shape
    groups = LANES // kcols
    half = n_row // 2 if n_row >= 4 and n_row & (n_row - 1) == 0 else n_row
    far_tiles = ut_ref.shape[0] // TILE
    chunks = 4 if far_tiles % 4 == 0 else 1
    n_near = near_ref.shape[0]
    n_parts = 4 if n_near % 4 == 0 else 1
    rank_max = ut_ref.shape[0] // rank_ref.shape[0]

    pair = 2 if n_row % 2 == 0 else 1
    low, high = lax.rem(row, pair), row // pair
    n_low, n_high = n_col * pair, n_row // pair
    peers = [(partner(row, d, n_row), col) for d in range(1, n_row)]
    peers += [(row, partner(col, d, n_col)) for d in range(1, n_col)]
    barrier = pltpu.get_barrier_semaphore()
    for peer in peers:
        pl.semaphore_signal(barrier, inc=1, device_id=peer, device_id_type=MESH)

    size = n_near // n_parts
    parts = [pl.ds(i * size, size) for i in range(n_parts)]
    moves = (
        (q_hbm, ag_refs[0].at[row]),
        (rank_hbm, rank_ref),
        (fr_hbm, fr_ref),
        (fc_hbm, fc_ref),
        (nr_hbm, nr_ref),
        (nc_hbm, nc_ref),
        (scale_hbm, scale_ref),
        *((near_hbm.at[part], near_ref.at[part]) for part in parts),
        (vt_hbm, vt_ref),
        (ut_hbm, ut_ref),
    )
    loads = [
        pltpu.make_async_copy(src, dst, load_sem.at[i]) for i, (src, dst) in enumerate(moves)
    ]
    for copy in loads:
        copy.start()

    def ag_copy(t, peer, late):
        return pltpu.make_async_remote_copy(
            src_ref=ag_refs[t].at[row],
            dst_ref=ag_refs[t].at[row],
            send_sem=ag_send.at[t, late],
            recv_sem=ag_recv.at[t, late],
            device_id=(peer, col),
            device_id_type=MESH,
        )

    def gather_start(t):
        for d in sorted(range(1, n_row), key=lambda d: (d == 1, (d + 1) % 2, -d)):
            ag_copy(t, partner(row, d, n_row), int(d >= half)).start()

    def wait_like(view, sem):
        pltpu.make_async_copy(view, view, sem).wait()

    def gather_wait(t, late):
        count = n_row - half if late else half - 1
        if count:
            view = ag_refs[t].at[pl.ds(0, count)]
            wait_like(view, ag_send.at[t, late])
            wait_like(view, ag_recv.at[t, late])

    def scatter_start(t):
        for d in sorted(range(1, n_col), key=lambda d: (d % 2, -d)):
            peer = partner(col, d, n_col)
            pltpu.make_async_remote_copy(
                src_ref=out_ref.at[t, peer],
                dst_ref=rs_ref.at[t, d - 1],
                send_sem=rs_send.at[t],
                recv_sem=rs_recv.at[t],
                device_id=(row, peer),
                device_id_type=MESH,
            ).start()

    def scatter_wait(t):
        view = rs_ref.at[t]
        wait_like(view, rs_send.at[t])
        wait_like(view, rs_recv.at[t])

    def gram_low_start(t, value):
        mine = low * n_col + col
        ga_ref[t, mine] = value
        for e in range(pair - 1, -1, -1):
            for d in range(n_col - 1, -1, -1):
                if (d, e) == (0, 0):
                    continue
                pltpu.make_async_remote_copy(
                    src_ref=ga_ref.at[t, mine],
                    dst_ref=ga_ref.at[t, mine],
                    send_sem=ga_send.at[t],
                    recv_sem=ga_recv.at[t],
                    device_id=(
                        high * pair + lax.rem(low + e, pair),
                        lax.rem(col + d, n_col),
                    ),
                    device_id_type=MESH,
                ).start()

    def gram_high_start(t):
        view = ga_ref.at[t, pl.ds(0, n_low - 1)]
        wait_like(view, ga_send.at[t])
        wait_like(view, ga_recv.at[t])
        gb_ref[t, high] = jnp.sum(ga_ref[t], axis=0)
        for d in range(n_high - 1, 0, -1):
            pltpu.make_async_remote_copy(
                src_ref=gb_ref.at[t, high],
                dst_ref=gb_ref.at[t, high],
                send_sem=gb_send.at[t],
                recv_sem=gb_recv.at[t],
                device_id=(partner(high, d, n_high) * pair + low, col),
                device_id_type=MESH,
            ).start()

    def gram_all(value):
        mine = row * n_col + col
        gd_ref[mine] = value
        for e in range(n_row - 1, -1, -1):
            for d in range(n_col - 1, -1, -1):
                if (d, e) == (0, 0):
                    continue
                pltpu.make_async_remote_copy(
                    src_ref=gd_ref.at[mine],
                    dst_ref=gd_ref.at[mine],
                    send_sem=gd_sem.at[0],
                    recv_sem=gd_sem.at[1],
                    device_id=(partner(row, e, n_row), partner(col, d, n_col)),
                    device_id_type=MESH,
                ).start()
        view = gd_ref.at[pl.ds(0, n_row * n_col - 1)]
        wait_like(view, gd_sem.at[0])
        wait_like(view, gd_sem.at[1])
        return jnp.sum(gd_ref[...], axis=0)

    def gram_wait(t):
        view = gb_ref.at[t, pl.ds(0, n_high - 1)]
        wait_like(view, gb_send.at[t])
        wait_like(view, gb_recv.at[t])
        return jnp.sum(gb_ref[t], axis=0)

    def selectors():
        place = lax.broadcasted_iota(jnp.int32, (SUB, TILE), 1)
        owner, rank_of = place // rank_max, lax.rem(place, rank_max)

        def tile(i, carry):
            fc = jnp.zeros((SUB, TILE), jnp.int32)
            fr, keep = fc, fc
            for j in range(TILE // rank_max):
                b = i * (TILE // rank_max) + j
                fc = jnp.where(owner == j, fc_ref[b], fc)
                fr = jnp.where(owner == j, fr_ref[b], fr)
                keep = jnp.where(owner == j, rank_ref[b], keep)
            start = pl.multiple_of(i * TILE, TILE)
            sel_ref[0, :, pl.ds(start, TILE)] = jnp.where(rank_of < keep, fc, -1)
            sel_ref[1, :, pl.ds(start, TILE)] = fr
            return carry

        lax.fori_loop(0, far_tiles, tile, 0)

    def far_inner(t, late, i):
        first = lax.rem(row // half + late, n_row // half) * half
        q_half = ag_refs[t][pl.ds(first, half)].reshape(half * kcols, leaf)
        tile = slice(i * TILE, (i + 1) * TILE)
        y = jnp.dot(q_half, vt_t_ref[:, tile], preferred_element_type=jnp.float32)
        fc = jnp.concatenate([sel_ref[0, :, tile]] * (kcols // SUB), axis=0) - first
        inner = inner_ref[:, tile] if late else jnp.zeros((kcols, TILE), jnp.float32)
        for c in range(half):
            inner = jnp.where(fc == c, y[c * kcols : (c + 1) * kcols, :], inner)
        return inner

    def far_early(t):
        if half < n_row:
            for i in range(far_tiles):
                inner_ref[:, i * TILE : (i + 1) * TILE] = far_inner(t, 0, i)

    def operator(t):
        def far_tile(i):
            tile = slice(i * TILE, (i + 1) * TILE)
            inner = far_inner(t, int(half < n_row), i)
            fr = jnp.concatenate([sel_ref[1, :, tile]] * (kcols // SUB), axis=0)
            for r in range(n_col):
                lhs_ref[r * kcols : (r + 1) * kcols, tile] = jnp.where(
                    fr == r, inner, 0.0
                ).astype(jnp.bfloat16)

        def near_block(b, acc):
            z = jnp.dot(ag_refs[t][nc_ref[b]], near_ref[b], preferred_element_type=jnp.float32)
            r_of = nr_ref[b]
            return [
                a + z * jnp.where(r_of == r, 1.0, 0.0).astype(jnp.float32)
                for r, a in enumerate(acc)
            ]

        def far_chunk(g):
            chunk = slice(g * far_tiles // chunks * TILE, (g + 1) * far_tiles // chunks * TILE)
            far = jnp.dot(lhs_ref[:, chunk], ut_ref[chunk, :], preferred_element_type=jnp.float32)
            for r in range(n_col):
                piece = far[r * kcols : (r + 1) * kcols, :]
                part_ref[t, r] = part_ref[t, r] + piece if g else piece

        near = [jnp.zeros((kcols, leaf), jnp.float32)] * n_col
        done = 0
        for i in range(far_tiles):
            far_tile(i)
            for b in range(i * n_near // far_tiles, (i + 1) * n_near // far_tiles):
                near = near_block(b, near)
            if (done + 1) * far_tiles // chunks <= i + 1 - 1:
                far_chunk(done)
                done += 1
        while done < chunks:
            far_chunk(done)
            done += 1
        for r in range(n_col):
            whole = part_ref[t, r] + near[r]
            part_ref[t, r] = whole
            out_ref[t, r] = whole.astype(jnp.bfloat16)

    lane = lax.broadcasted_iota(jnp.int32, (SUB, LANES), 1)
    lane_full = lax.broadcasted_iota(jnp.int32, (kcols, LANES), 1)
    sub_full = lax.broadcasted_iota(jnp.int32, (kcols, LANES), 0)

    def pack_gram(product):
        tiled = jnp.concatenate([product] * groups, axis=0)
        g = dot_nt(product, tiled, HIGH)
        rows = kcols // groups
        packed = jnp.zeros((rows, LANES), jnp.float32)
        for i in range(groups):
            packed = jnp.where(lane // kcols == i, g[i * rows : (i + 1) * rows, :], packed)
        return packed

    def solve(g):
        g = g / total_pts
        parts = []
        for i in range(groups):
            shift = (1 - i) * kcols % LANES
            parts.append(pltpu.roll(g, shift, 1) if shift else g)
        s = jnp.concatenate(parts, axis=0)
        work = jnp.where(lane_full < kcols, jnp.where(lane_full == sub_full, 1.0, 0.0), s)
        work = jnp.where(lane_full < 2 * kcols, work, 0.0)
        return factorize(work, kcols)


    loads[0].wait()
    pl.semaphore_wait(barrier, len(peers))
    gather_start(0)
    for copy in loads[1:4]:
        copy.wait()
    selectors()
    for i in range(n_parts):
        loads[7 + i].wait()
        for b in range(i * size, (i + 1) * size):
            near_ref[b] = near_ref[b].T
    loads[7 + n_parts].wait()
    for i in range(far_tiles):
        tile = slice(i * TILE, (i + 1) * TILE)
        vt_t_ref[:, tile] = vt_ref[tile, :].T
    for copy in (*loads[4:7], loads[8 + n_parts]):
        copy.wait()
    for t in range(ITERS):
        if t > 0:
            gram_high_start(t - 1)
        gather_wait(t, 0)
        far_early(t)
        gather_wait(t, 1)
        operator(t)
        scatter_start(t)
        if t > 0:
            rows = solve(gram_wait(t - 1))
        scatter_wait(t)
        total = part_ref[t, col]
        for d in range(1, n_col):
            total = total + rs_ref[t, d - 1].astype(jnp.float32)
        product = total * scale_ref[...]
        if t > 0:
            product = apply_inverse(rows, product)
        if t < ITERS - 1:
            ag_refs[t + 1][row] = product.astype(jnp.bfloat16)
            gather_start(t + 1)
            gram_low_start(t, pack_gram(product))
    prod_ref[...] = product
    rows_ref[...] = solve(gram_all(pack_gram(product)))


def on_device(
    q_start,
    row_scale,
    near_blocks,
    near_rows,
    near_cols,
    far_ut,
    far_vt,
    far_rank,
    far_rows,
    far_cols,
):
    leaf, kcols = q_start.shape
    n_row = lax.axis_size("row")
    n_col = lax.axis_size("col")
    n_dev = n_row * n_col
    pair = 2 if n_row % 2 == 0 else 1
    n_low, n_high = n_col * pair, n_row // pair
    n_near = near_blocks.shape[1]
    n_far, rank_max = far_ut.shape[1:3]
    near = near_blocks[0]
    ut = far_ut.reshape(n_far * rank_max, leaf)
    vt = far_vt.reshape(n_far * rank_max, leaf)
    vmem = pl.BlockSpec(memory_space=pltpu.VMEM)
    hbm = pl.BlockSpec(memory_space=pl.ANY)
    f32, bf16 = jnp.float32, jnp.bfloat16
    rows, product = pl.pallas_call(
        functools.partial(kernel, n_row, n_col, leaf * n_dev),
        name="subspace",
        out_shape=(
            pltpu.VMEM((kcols, LANES), f32),
            pltpu.VMEM((kcols, leaf), f32),
        ),
        in_specs=[hbm] * 10,
        out_specs=(vmem, vmem),
        scratch_shapes=[
            pltpu.VMEM((1, leaf), f32),
            pltpu.SMEM((n_far,), jnp.int32),
            pltpu.SMEM((n_far,), jnp.int32),
            pltpu.SMEM((n_far,), jnp.int32),
            pltpu.SMEM((n_near,), jnp.int32),
            pltpu.SMEM((n_near,), jnp.int32),
            pltpu.VMEM(near.shape, bf16),
            pltpu.VMEM(ut.shape, bf16),
            pltpu.VMEM(vt.shape, bf16),
            [pltpu.VMEM((n_row, kcols, leaf), bf16) for _ in range(ITERS)],
            pltpu.VMEM((2, SUB, n_far * rank_max), jnp.int32),
            pltpu.VMEM((kcols, n_far * rank_max), f32),
            pltpu.VMEM((n_col * kcols, n_far * rank_max), bf16),
            pltpu.VMEM((leaf, n_far * rank_max), bf16),
            pltpu.VMEM((ITERS, n_col, kcols, leaf), f32),
            pltpu.VMEM((ITERS, n_col, kcols, leaf), bf16),
            pltpu.VMEM((ITERS, n_col - 1, kcols, leaf), bf16),
            pltpu.VMEM((ITERS - 1, n_low, kcols * kcols // LANES, LANES), f32),
            pltpu.VMEM((ITERS - 1, n_high, kcols * kcols // LANES, LANES), f32),
            pltpu.VMEM((n_dev, kcols * kcols // LANES, LANES), f32),
            pltpu.SemaphoreType.DMA((13,)),
            pltpu.SemaphoreType.DMA((ITERS, 2)),
            pltpu.SemaphoreType.DMA((ITERS, 2)),
            pltpu.SemaphoreType.DMA((ITERS,)),
            pltpu.SemaphoreType.DMA((ITERS,)),
            pltpu.SemaphoreType.DMA((ITERS,)),
            pltpu.SemaphoreType.DMA((ITERS,)),
            pltpu.SemaphoreType.DMA((ITERS,)),
            pltpu.SemaphoreType.DMA((ITERS,)),
            pltpu.SemaphoreType.DMA((2,)),
        ],
        compiler_params=pltpu.CompilerParams(
            collective_id=0, has_side_effects=True, vmem_limit_bytes=56 * 1024 * 1024
        ),
    )(
        q_start.T,
        row_scale.reshape(1, leaf),
        far_rank[0, 0],
        far_rows[0, 0],
        far_cols[0, 0],
        near_rows[0, 0],
        near_cols[0, 0],
        near,
        ut,
        vt,
    )
    basis_t, factor = pl.pallas_call(
        finish,
        name="finish",
        out_shape=(
            jax.ShapeDtypeStruct((kcols, leaf), f32),
            jax.ShapeDtypeStruct((kcols, kcols), f32),
        ),
        in_specs=[vmem, vmem],
        out_specs=(vmem, vmem),
    )(*(pltpu.with_memory_space_constraint(x, pltpu.VMEM) for x in (rows, product)))
    return basis_t.T, factor


def solution(mesh):
    in_specs = (
        P(("row", "col"), None),
        P(("row", "col")),
        P("row", "col", None, None),
        P("row", "col", None),
        P("row", "col", None),
        P("row", "col", None, None),
        P("row", "col", None, None),
        P("row", "col", None),
        P("row", "col", None),
        P("row", "col", None),
    )
    out_specs = (P(("row", "col"), None), P())
    return jax.shard_map(
        on_device, mesh=mesh, in_specs=in_specs, out_specs=out_specs, check_vma=False
    )
```

```python
import functools

import jax
import jax.numpy as jnp
from jax import lax
from jax.experimental import pallas as pl
from jax.experimental.pallas import tpu as pltpu
from jax.sharding import PartitionSpec as P

ITERS = 4
MESH = pl.DeviceIdType.MESH
HIGH = lax.Precision.HIGHEST
NT = (((1,), (1,)), ((), ()))
LANES = 128
SUB = 8
TILE = 256


def dot_nt(a, b, precision=None):
    return lax.dot_general(a, b, NT, precision=precision, preferred_element_type=jnp.float32)


def partner(index, step, size):
    if size & (size - 1):
        return lax.rem(index + step, size)
    out, bit = 0, 1
    while bit < size:
        mine = (index // bit) % 2
        out = out + bit * (1 - mine if step & bit else mine)
        bit *= 2
    return out


def factorize(work, kcols):
    blocks = kcols // SUB
    w = [work[SUB * q : SUB * (q + 1), :] for q in range(blocks)]
    sub = lax.broadcasted_iota(jnp.int32, (SUB, LANES), 0)
    diag = []
    for p in range(blocks):
        cb = [
            [
                jnp.broadcast_to(w[q][:, kcols + SUB * p + j : kcols + SUB * p + j + 1], (SUB, LANES))
                if q >= p
                else None
                for q in range(blocks)
            ]
            for j in range(SUB)
        ]
        dp = jnp.ones((SUB, LANES), jnp.float32)
        for j in range(SUB):
            d = jnp.broadcast_to(cb[j][p][j : j + 1, :], (SUB, LANES))
            dp = jnp.where(sub == j, d, dp)
            inv = 1.0 / d
            row = jnp.broadcast_to(w[p][j : j + 1, :], (SUB, LANES)) * inv
            others = {
                k: jnp.broadcast_to(cb[k][p][j : j + 1, :], (SUB, LANES)) * inv
                for k in range(j + 1, SUB)
            }
            for q in range(p, blocks):
                m = cb[j][q]
                if q == p:
                    m = jnp.where(sub > j, m, 0.0)
                w[q] = w[q] - m * row
                for k in range(j + 1, SUB):
                    cb[k][q] = cb[k][q] - m * others[k]
        diag.append(dp)
    return jnp.concatenate([w[q] * lax.rsqrt(diag[q]) for q in range(blocks)], axis=0)


def apply_inverse(rows, product):
    pad = jnp.zeros((LANES - product.shape[0], product.shape[1]), jnp.float32)
    return jnp.dot(
        rows,
        jnp.concatenate([product, pad], axis=0),
        precision=HIGH,
        preferred_element_type=jnp.float32,
    )


def finish(rows_ref, prod_ref, basis_ref, factor_ref):
    rows = rows_ref[...]
    kcols = rows.shape[0]
    lane = lax.broadcasted_iota(jnp.int32, rows.shape, 1)
    sub = lax.broadcasted_iota(jnp.int32, rows.shape, 0)
    basis_ref[...] = apply_inverse(rows, prod_ref[...])
    upper = jnp.where(lane - kcols >= sub, rows, 0.0)
    pick = jnp.where(lane == sub + kcols, 1.0, 0.0).astype(jnp.float32)
    factor_ref[...] = dot_nt(pick, upper, HIGH)


def kernel(
    n_row,
    n_col,
    total_pts,
    q_hbm,
    scale_hbm,
    rank_hbm,
    fr_hbm,
    fc_hbm,
    nr_hbm,
    nc_hbm,
    near_hbm,
    ut_hbm,
    vt_hbm,
    rows_ref,
    prod_ref,
    scale_ref,
    rank_ref,
    fr_ref,
    fc_ref,
    nr_ref,
    nc_ref,
    near_ref,
    ut_ref,
    vt_ref,
    ag_refs,
    sel_ref,
    inner_ref,
    lhs_ref,
    vt_t_ref,
    part_ref,
    out_ref,
    rs_ref,
    ga_ref,
    gb_ref,
    gd_ref,
    load_sem,
    ag_send,
    ag_recv,
    rs_send,
    rs_recv,
    ga_send,
    ga_recv,
    gb_send,
    gb_recv,
    gd_sem,
):
    row = lax.axis_index("row")
    col = lax.axis_index("col")
    kcols, leaf = q_hbm.shape
    groups = LANES // kcols
    half = n_row // 2 if n_row >= 4 and n_row & (n_row - 1) == 0 else n_row
    far_tiles = ut_ref.shape[0] // TILE
    chunks = 4 if far_tiles % 4 == 0 else 1
    n_near = near_ref.shape[0]
    n_parts = 4 if n_near % 4 == 0 else 1
    rank_max = ut_ref.shape[0] // rank_ref.shape[0]

    pair = 2 if n_row % 2 == 0 else 1
    low, high = lax.rem(row, pair), row // pair
    n_low, n_high = n_col * pair, n_row // pair
    peers = [(partner(row, d, n_row), col) for d in range(1, n_row)]
    peers += [(row, partner(col, d, n_col)) for d in range(1, n_col)]
    barrier = pltpu.get_barrier_semaphore()
    for peer in peers:
        pl.semaphore_signal(barrier, inc=1, device_id=peer, device_id_type=MESH)

    size = n_near // n_parts
    parts = [pl.ds(i * size, size) for i in range(n_parts)]
    moves = (
        (q_hbm, ag_refs[0].at[row]),
        (rank_hbm, rank_ref),
        (fr_hbm, fr_ref),
        (fc_hbm, fc_ref),
        (nr_hbm, nr_ref),
        (nc_hbm, nc_ref),
        (scale_hbm, scale_ref),
        *((near_hbm.at[part], near_ref.at[part]) for part in parts),
        (vt_hbm, vt_ref),
        (ut_hbm, ut_ref),
    )
    loads = [
        pltpu.make_async_copy(src, dst, load_sem.at[i]) for i, (src, dst) in enumerate(moves)
    ]
    for copy in loads:
        copy.start()

    def ag_copy(t, peer, late):
        return pltpu.make_async_remote_copy(
            src_ref=ag_refs[t].at[row],
            dst_ref=ag_refs[t].at[row],
            send_sem=ag_send.at[t, late],
            recv_sem=ag_recv.at[t, late],
            device_id=(peer, col),
            device_id_type=MESH,
        )

    def gather_start(t):
        for d in sorted(range(1, n_row), key=lambda d: (d == 1, (d + 1) % 2, -d)):
            ag_copy(t, partner(row, d, n_row), int(d >= half)).start()

    def wait_like(view, sem):
        pltpu.make_async_copy(view, view, sem).wait()

    def gather_wait(t, late):
        count = n_row - half if late else half - 1
        if count:
            view = ag_refs[t].at[pl.ds(0, count)]
            wait_like(view, ag_send.at[t, late])
            wait_like(view, ag_recv.at[t, late])

    def scatter_start(t):
        for d in sorted(range(1, n_col), key=lambda d: (d % 2, -d)):
            peer = partner(col, d, n_col)
            pltpu.make_async_remote_copy(
                src_ref=out_ref.at[t, peer],
                dst_ref=rs_ref.at[t, d - 1],
                send_sem=rs_send.at[t],
                recv_sem=rs_recv.at[t],
                device_id=(row, peer),
                device_id_type=MESH,
            ).start()

    def scatter_wait(t):
        view = rs_ref.at[t]
        wait_like(view, rs_send.at[t])
        wait_like(view, rs_recv.at[t])

    def gram_low_start(t, value):
        mine = low * n_col + col
        ga_ref[t, mine] = value
        for d in sorted(range(n_col), key=lambda d: (-(d // 2), d % 2)):
            for e in range(pair - 1, -1, -1):
                if (d, e) == (0, 0):
                    continue
                pltpu.make_async_remote_copy(
                    src_ref=ga_ref.at[t, mine],
                    dst_ref=ga_ref.at[t, mine],
                    send_sem=ga_send.at[t],
                    recv_sem=ga_recv.at[t],
                    device_id=(
                        high * pair + lax.rem(low + e, pair),
                        partner(col, d, n_col),
                    ),
                    device_id_type=MESH,
                ).start()

    def gram_high_start(t):
        view = ga_ref.at[t, pl.ds(0, n_low - 1)]
        wait_like(view, ga_send.at[t])
        wait_like(view, ga_recv.at[t])
        gb_ref[t, high] = jnp.sum(ga_ref[t], axis=0)
        for d in range(n_high - 1, 0, -1):
            pltpu.make_async_remote_copy(
                src_ref=gb_ref.at[t, high],
                dst_ref=gb_ref.at[t, high],
                send_sem=gb_send.at[t],
                recv_sem=gb_recv.at[t],
                device_id=(partner(high, d, n_high) * pair + low, col),
                device_id_type=MESH,
            ).start()

    def gram_all(value):
        mine = row * n_col + col
        gd_ref[mine] = value
        for d in sorted(range(n_col), key=lambda d: (-(d // 2), d % 2)):
            for e in sorted(range(n_row), key=lambda e: (e < 2, (e + 1) % 2, -e)):
                if (d, e) == (0, 0):
                    continue
                pltpu.make_async_remote_copy(
                    src_ref=gd_ref.at[mine],
                    dst_ref=gd_ref.at[mine],
                    send_sem=gd_sem.at[0],
                    recv_sem=gd_sem.at[1],
                    device_id=(partner(row, e, n_row), partner(col, d, n_col)),
                    device_id_type=MESH,
                ).start()
        view = gd_ref.at[pl.ds(0, n_row * n_col - 1)]
        wait_like(view, gd_sem.at[0])
        wait_like(view, gd_sem.at[1])
        return jnp.sum(gd_ref[...], axis=0)

    def gram_wait(t):
        view = gb_ref.at[t, pl.ds(0, n_high - 1)]
        wait_like(view, gb_send.at[t])
        wait_like(view, gb_recv.at[t])
        return jnp.sum(gb_ref[t], axis=0)

    def selectors():
        place = lax.broadcasted_iota(jnp.int32, (SUB, TILE), 1)
        owner, rank_of = place // rank_max, lax.rem(place, rank_max)

        def tile(i, carry):
            fc = jnp.zeros((SUB, TILE), jnp.int32)
            fr, keep = fc, fc
            for j in range(TILE // rank_max):
                b = i * (TILE // rank_max) + j
                fc = jnp.where(owner == j, fc_ref[b], fc)
                fr = jnp.where(owner == j, fr_ref[b], fr)
                keep = jnp.where(owner == j, rank_ref[b], keep)
            start = pl.multiple_of(i * TILE, TILE)
            sel_ref[0, :, pl.ds(start, TILE)] = jnp.where(rank_of < keep, fc, -1)
            sel_ref[1, :, pl.ds(start, TILE)] = fr
            return carry

        lax.fori_loop(0, far_tiles, tile, 0)

    def far_inner(t, late, i):
        first = lax.rem(row // half + late, n_row // half) * half
        q_half = ag_refs[t][pl.ds(first, half)].reshape(half * kcols, leaf)
        tile = slice(i * TILE, (i + 1) * TILE)
        y = jnp.dot(q_half, vt_t_ref[:, tile], preferred_element_type=jnp.float32)
        fc = jnp.concatenate([sel_ref[0, :, tile]] * (kcols // SUB), axis=0) - first
        inner = inner_ref[:, tile] if late else jnp.zeros((kcols, TILE), jnp.float32)
        for c in range(half):
            inner = jnp.where(fc == c, y[c * kcols : (c + 1) * kcols, :], inner)
        return inner

    def far_early(t):
        if half < n_row:
            for i in range(far_tiles):
                inner_ref[:, i * TILE : (i + 1) * TILE] = far_inner(t, 0, i)

    def operator(t):
        def far_tile(i):
            tile = slice(i * TILE, (i + 1) * TILE)
            inner = far_inner(t, int(half < n_row), i)
            fr = jnp.concatenate([sel_ref[1, :, tile]] * (kcols // SUB), axis=0)
            for r in range(n_col):
                lhs_ref[r * kcols : (r + 1) * kcols, tile] = jnp.where(
                    fr == r, inner, 0.0
                ).astype(jnp.bfloat16)

        def near_block(b, acc):
            z = jnp.dot(ag_refs[t][nc_ref[b]], near_ref[b], preferred_element_type=jnp.float32)
            r_of = nr_ref[b]
            return [
                a + z * jnp.where(r_of == r, 1.0, 0.0).astype(jnp.float32)
                for r, a in enumerate(acc)
            ]

        def far_chunk(g):
            chunk = slice(g * far_tiles // chunks * TILE, (g + 1) * far_tiles // chunks * TILE)
            far = jnp.dot(lhs_ref[:, chunk], ut_ref[chunk, :], preferred_element_type=jnp.float32)
            for r in range(n_col):
                piece = far[r * kcols : (r + 1) * kcols, :]
                part_ref[t, r] = part_ref[t, r] + piece if g else piece

        near = [jnp.zeros((kcols, leaf), jnp.float32)] * n_col
        done = 0
        n_early = n_near // 2
        for i in range(far_tiles):
            far_tile(i)
            for b in range(i * n_early // far_tiles, (i + 1) * n_early // far_tiles):
                near = near_block(b, near)
            if (done + 1) * far_tiles // chunks <= i + 1 - 1:
                far_chunk(done)
                done += 1
        while done < chunks:
            far_chunk(done)
            done += 1
        for b in range(n_early, n_near):
            near = near_block(b, near)
        for r in range(n_col):
            whole = part_ref[t, r] + near[r]
            part_ref[t, r] = whole
            out_ref[t, r] = whole.astype(jnp.bfloat16)

    lane = lax.broadcasted_iota(jnp.int32, (SUB, LANES), 1)
    lane_full = lax.broadcasted_iota(jnp.int32, (kcols, LANES), 1)
    sub_full = lax.broadcasted_iota(jnp.int32, (kcols, LANES), 0)

    def pack_gram(product):
        tiled = jnp.concatenate([product] * groups, axis=0)
        g = dot_nt(product, tiled, HIGH)
        rows = kcols // groups
        packed = jnp.zeros((rows, LANES), jnp.float32)
        for i in range(groups):
            packed = jnp.where(lane // kcols == i, g[i * rows : (i + 1) * rows, :], packed)
        return packed

    def solve(g):
        g = g / total_pts
        parts = []
        for i in range(groups):
            shift = (1 - i) * kcols % LANES
            parts.append(pltpu.roll(g, shift, 1) if shift else g)
        s = jnp.concatenate(parts, axis=0)
        work = jnp.where(lane_full < kcols, jnp.where(lane_full == sub_full, 1.0, 0.0), s)
        work = jnp.where(lane_full < 2 * kcols, work, 0.0)
        return factorize(work, kcols)


    loads[0].wait()
    pl.semaphore_wait(barrier, len(peers))
    gather_start(0)
    for copy in loads[1:4]:
        copy.wait()
    selectors()
    for i in range(n_parts):
        loads[7 + i].wait()
        for b in range(i * size, (i + 1) * size):
            near_ref[b] = near_ref[b].T
    loads[7 + n_parts].wait()
    for i in range(far_tiles):
        tile = slice(i * TILE, (i + 1) * TILE)
        vt_t_ref[:, tile] = vt_ref[tile, :].T
    for copy in (*loads[4:7], loads[8 + n_parts]):
        copy.wait()
    for t in range(ITERS):
        if t > 0:
            gram_high_start(t - 1)
        gather_wait(t, 0)
        far_early(t)
        gather_wait(t, 1)
        operator(t)
        scatter_start(t)
        if t > 0:
            rows = solve(gram_wait(t - 1))
        scatter_wait(t)
        total = part_ref[t, col]
        for d in range(1, n_col):
            total = total + rs_ref[t, d - 1].astype(jnp.float32)
        product = total * scale_ref[...]
        if t > 0:
            product = apply_inverse(rows, product)
        if t < ITERS - 1:
            ag_refs[t + 1][row] = product.astype(jnp.bfloat16)
            gather_start(t + 1)
            gram_low_start(t, pack_gram(product))
    prod_ref[...] = product
    rows_ref[...] = solve(gram_all(pack_gram(product)))


def on_device(
    q_start,
    row_scale,
    near_blocks,
    near_rows,
    near_cols,
    far_ut,
    far_vt,
    far_rank,
    far_rows,
    far_cols,
):
    leaf, kcols = q_start.shape
    n_row = lax.axis_size("row")
    n_col = lax.axis_size("col")
    n_dev = n_row * n_col
    pair = 2 if n_row % 2 == 0 else 1
    n_low, n_high = n_col * pair, n_row // pair
    n_near = near_blocks.shape[1]
    n_far, rank_max = far_ut.shape[1:3]
    near = near_blocks[0]
    ut = far_ut.reshape(n_far * rank_max, leaf)
    vt = far_vt.reshape(n_far * rank_max, leaf)
    vmem = pl.BlockSpec(memory_space=pltpu.VMEM)
    hbm = pl.BlockSpec(memory_space=pl.ANY)
    f32, bf16 = jnp.float32, jnp.bfloat16
    rows, product = pl.pallas_call(
        functools.partial(kernel, n_row, n_col, leaf * n_dev),
        name="subspace",
        out_shape=(
            pltpu.VMEM((kcols, LANES), f32),
            pltpu.VMEM((kcols, leaf), f32),
        ),
        in_specs=[hbm] * 10,
        out_specs=(vmem, vmem),
        scratch_shapes=[
            pltpu.VMEM((1, leaf), f32),
            pltpu.SMEM((n_far,), jnp.int32),
            pltpu.SMEM((n_far,), jnp.int32),
            pltpu.SMEM((n_far,), jnp.int32),
            pltpu.SMEM((n_near,), jnp.int32),
            pltpu.SMEM((n_near,), jnp.int32),
            pltpu.VMEM(near.shape, bf16),
            pltpu.VMEM(ut.shape, bf16),
            pltpu.VMEM(vt.shape, bf16),
            [pltpu.VMEM((n_row, kcols, leaf), bf16) for _ in range(ITERS)],
            pltpu.VMEM((2, SUB, n_far * rank_max), jnp.int32),
            pltpu.VMEM((kcols, n_far * rank_max), f32),
            pltpu.VMEM((n_col * kcols, n_far * rank_max), bf16),
            pltpu.VMEM((leaf, n_far * rank_max), bf16),
            pltpu.VMEM((ITERS, n_col, kcols, leaf), f32),
            pltpu.VMEM((ITERS, n_col, kcols, leaf), bf16),
            pltpu.VMEM((ITERS, n_col - 1, kcols, leaf), bf16),
            pltpu.VMEM((ITERS - 1, n_low, kcols * kcols // LANES, LANES), f32),
            pltpu.VMEM((ITERS - 1, n_high, kcols * kcols // LANES, LANES), f32),
            pltpu.VMEM((n_dev, kcols * kcols // LANES, LANES), f32),
            pltpu.SemaphoreType.DMA((13,)),
            pltpu.SemaphoreType.DMA((ITERS, 2)),
            pltpu.SemaphoreType.DMA((ITERS, 2)),
            pltpu.SemaphoreType.DMA((ITERS,)),
            pltpu.SemaphoreType.DMA((ITERS,)),
            pltpu.SemaphoreType.DMA((ITERS,)),
            pltpu.SemaphoreType.DMA((ITERS,)),
            pltpu.SemaphoreType.DMA((ITERS,)),
            pltpu.SemaphoreType.DMA((ITERS,)),
            pltpu.SemaphoreType.DMA((2,)),
        ],
        compiler_params=pltpu.CompilerParams(
            collective_id=0, has_side_effects=True, vmem_limit_bytes=56 * 1024 * 1024
        ),
    )(
        q_start.T,
        row_scale.reshape(1, leaf),
        far_rank[0, 0],
        far_rows[0, 0],
        far_cols[0, 0],
        near_rows[0, 0],
        near_cols[0, 0],
        near,
        ut,
        vt,
    )
    basis_t, factor = pl.pallas_call(
        finish,
        name="finish",
        out_shape=(
            jax.ShapeDtypeStruct((kcols, leaf), f32),
            jax.ShapeDtypeStruct((kcols, kcols), f32),
        ),
        in_specs=[vmem, vmem],
        out_specs=(vmem, vmem),
    )(*(pltpu.with_memory_space_constraint(x, pltpu.VMEM) for x in (rows, product)))
    return basis_t.T, factor


def solution(mesh):
    in_specs = (
        P(("row", "col"), None),
        P(("row", "col")),
        P("row", "col", None, None),
        P("row", "col", None),
        P("row", "col", None),
        P("row", "col", None, None),
        P("row", "col", None, None),
        P("row", "col", None),
        P("row", "col", None),
        P("row", "col", None),
    )
    out_specs = (P(("row", "col"), None), P())
    return jax.shard_map(
        on_device, mesh=mesh, in_specs=in_specs, out_specs=out_specs, check_vma=False
    )
```

```python
import functools

import jax
import jax.numpy as jnp
from jax import lax
from jax.experimental import pallas as pl
from jax.experimental.pallas import tpu as pltpu
from jax.sharding import PartitionSpec as P

ITERS = 4
MESH = pl.DeviceIdType.MESH
HIGH = lax.Precision.HIGHEST
NT = (((1,), (1,)), ((), ()))
LANES = 128
SUB = 8
TILE = 256


def dot_nt(a, b, precision=None):
    return lax.dot_general(a, b, NT, precision=precision, preferred_element_type=jnp.float32)


def partner(index, step, size):
    if size & (size - 1):
        return lax.rem(index + step, size)
    out, bit = 0, 1
    while bit < size:
        mine = (index // bit) % 2
        out = out + bit * (1 - mine if step & bit else mine)
        bit *= 2
    return out


def factorize(work, kcols):
    blocks = kcols // SUB
    w = [work[SUB * q : SUB * (q + 1), :] for q in range(blocks)]
    sub = lax.broadcasted_iota(jnp.int32, (SUB, LANES), 0)
    diag = []
    for p in range(blocks):
        cb = [
            [
                jnp.broadcast_to(w[q][:, kcols + SUB * p + j : kcols + SUB * p + j + 1], (SUB, LANES))
                if q >= p
                else None
                for q in range(blocks)
            ]
            for j in range(SUB)
        ]
        dp = jnp.ones((SUB, LANES), jnp.float32)
        for j in range(SUB):
            d = jnp.broadcast_to(cb[j][p][j : j + 1, :], (SUB, LANES))
            dp = jnp.where(sub == j, d, dp)
            inv = 1.0 / d
            row = jnp.broadcast_to(w[p][j : j + 1, :], (SUB, LANES)) * inv
            others = {
                k: jnp.broadcast_to(cb[k][p][j : j + 1, :], (SUB, LANES)) * inv
                for k in range(j + 1, SUB)
            }
            for q in range(p, blocks):
                m = cb[j][q]
                if q == p:
                    m = jnp.where(sub > j, m, 0.0)
                w[q] = w[q] - m * row
                for k in range(j + 1, SUB):
                    cb[k][q] = cb[k][q] - m * others[k]
        diag.append(dp)
    return jnp.concatenate([w[q] * lax.rsqrt(diag[q]) for q in range(blocks)], axis=0)


def apply_inverse(rows, product):
    pad = jnp.zeros((LANES - product.shape[0], product.shape[1]), jnp.float32)
    return jnp.dot(
        rows,
        jnp.concatenate([product, pad], axis=0),
        precision=HIGH,
        preferred_element_type=jnp.float32,
    )


def finish(rows_ref, prod_ref, basis_ref, factor_ref):
    rows = rows_ref[...]
    kcols = rows.shape[0]
    lane = lax.broadcasted_iota(jnp.int32, rows.shape, 1)
    sub = lax.broadcasted_iota(jnp.int32, rows.shape, 0)
    basis_ref[...] = apply_inverse(rows, prod_ref[...])
    upper = jnp.where(lane - kcols >= sub, rows, 0.0)
    pick = jnp.where(lane == sub + kcols, 1.0, 0.0).astype(jnp.float32)
    factor_ref[...] = dot_nt(pick, upper, HIGH)


def kernel(
    n_row,
    n_col,
    total_pts,
    q_hbm,
    scale_hbm,
    rank_hbm,
    fr_hbm,
    fc_hbm,
    nr_hbm,
    nc_hbm,
    near_hbm,
    ut_hbm,
    vt_hbm,
    rows_ref,
    prod_ref,
    scale_ref,
    rank_ref,
    fr_ref,
    fc_ref,
    nr_ref,
    nc_ref,
    near_ref,
    ut_ref,
    vt_ref,
    ag_refs,
    sel_ref,
    inner_ref,
    lhs_ref,
    vt_t_ref,
    part_ref,
    out_ref,
    rs_ref,
    ga_ref,
    gb_ref,
    gd_ref,
    load_sem,
    ag_send,
    ag_recv,
    rs_send,
    rs_recv,
    ga_send,
    ga_recv,
    gb_send,
    gb_recv,
    gd_sem,
):
    row = lax.axis_index("row")
    col = lax.axis_index("col")
    kcols, leaf = q_hbm.shape
    groups = LANES // kcols
    half = n_row // 2 if n_row >= 4 and n_row & (n_row - 1) == 0 else n_row
    far_tiles = ut_ref.shape[0] // TILE
    chunks = 4 if far_tiles % 4 == 0 else 1
    n_near = near_ref.shape[0]
    n_parts = 4 if n_near % 4 == 0 else 1
    rank_max = ut_ref.shape[0] // rank_ref.shape[0]

    pair = 2 if n_row % 2 == 0 else 1
    low, high = lax.rem(row, pair), row // pair
    n_low, n_high = n_col * pair, n_row // pair
    peers = [(partner(row, d, n_row), col) for d in range(1, n_row)]
    peers += [(row, partner(col, d, n_col)) for d in range(1, n_col)]
    barrier = pltpu.get_barrier_semaphore()
    for peer in peers:
        pl.semaphore_signal(barrier, inc=1, device_id=peer, device_id_type=MESH)

    size = n_near // n_parts
    parts = [pl.ds(i * size, size) for i in range(n_parts)]
    moves = (
        (q_hbm, ag_refs[0].at[row]),
        (rank_hbm, rank_ref),
        (fr_hbm, fr_ref),
        (fc_hbm, fc_ref),
        (nr_hbm, nr_ref),
        (nc_hbm, nc_ref),
        (scale_hbm, scale_ref),
        *((near_hbm.at[part], near_ref.at[part]) for part in parts),
        (vt_hbm, vt_ref),
        (ut_hbm, ut_ref),
    )
    loads = [
        pltpu.make_async_copy(src, dst, load_sem.at[i]) for i, (src, dst) in enumerate(moves)
    ]
    for copy in loads:
        copy.start()

    def ag_copy(t, peer, late):
        return pltpu.make_async_remote_copy(
            src_ref=ag_refs[t].at[row],
            dst_ref=ag_refs[t].at[row],
            send_sem=ag_send.at[t, late],
            recv_sem=ag_recv.at[t, late],
            device_id=(peer, col),
            device_id_type=MESH,
        )

    def gather_start(t):
        for d in sorted(range(1, n_row), key=lambda d: (d == 1, (d + 1) % 2, -d)):
            ag_copy(t, partner(row, d, n_row), int(d >= half)).start()

    def wait_like(view, sem):
        pltpu.make_async_copy(view, view, sem).wait()

    def gather_wait(t, late):
        count = n_row - half if late else half - 1
        if count:
            view = ag_refs[t].at[pl.ds(0, count)]
            wait_like(view, ag_send.at[t, late])
            wait_like(view, ag_recv.at[t, late])

    def scatter_start(t):
        for d in sorted(range(1, n_col), key=lambda d: (d % 2, -d)):
            peer = partner(col, d, n_col)
            pltpu.make_async_remote_copy(
                src_ref=out_ref.at[t, peer],
                dst_ref=rs_ref.at[t, d - 1],
                send_sem=rs_send.at[t],
                recv_sem=rs_recv.at[t],
                device_id=(row, peer),
                device_id_type=MESH,
            ).start()

    def scatter_wait(t):
        view = rs_ref.at[t]
        wait_like(view, rs_send.at[t])
        wait_like(view, rs_recv.at[t])

    def gram_low_start(t, value):
        mine = low * n_col + col
        ga_ref[t, mine] = value
        for d in sorted(range(n_col), key=lambda d: (-(d // 2), d % 2)):
            for e in range(pair - 1, -1, -1):
                if (d, e) == (0, 0):
                    continue
                pltpu.make_async_remote_copy(
                    src_ref=ga_ref.at[t, mine],
                    dst_ref=ga_ref.at[t, mine],
                    send_sem=ga_send.at[t],
                    recv_sem=ga_recv.at[t],
                    device_id=(
                        high * pair + lax.rem(low + e, pair),
                        partner(col, d, n_col),
                    ),
                    device_id_type=MESH,
                ).start()

    def gram_high_start(t):
        view = ga_ref.at[t, pl.ds(0, n_low - 1)]
        wait_like(view, ga_send.at[t])
        wait_like(view, ga_recv.at[t])
        gb_ref[t, high] = jnp.sum(ga_ref[t], axis=0)
        for d in range(n_high - 1, 0, -1):
            pltpu.make_async_remote_copy(
                src_ref=gb_ref.at[t, high],
                dst_ref=gb_ref.at[t, high],
                send_sem=gb_send.at[t],
                recv_sem=gb_recv.at[t],
                device_id=(partner(high, d, n_high) * pair + low, col),
                device_id_type=MESH,
            ).start()

    def gram_all(value):
        mine = row * n_col + col
        gd_ref[mine] = value
        for d in sorted(range(n_col), key=lambda d: (-(d // 2), d % 2)):
            for e in sorted(range(n_row), key=lambda e: (e < 2, (e + 1) % 2, -e)):
                if (d, e) == (0, 0):
                    continue
                pltpu.make_async_remote_copy(
                    src_ref=gd_ref.at[mine],
                    dst_ref=gd_ref.at[mine],
                    send_sem=gd_sem.at[0],
                    recv_sem=gd_sem.at[1],
                    device_id=(partner(row, e, n_row), partner(col, d, n_col)),
                    device_id_type=MESH,
                ).start()
        view = gd_ref.at[pl.ds(0, n_row * n_col - 1)]
        wait_like(view, gd_sem.at[0])
        wait_like(view, gd_sem.at[1])
        return jnp.sum(gd_ref[...], axis=0)

    def gram_wait(t):
        view = gb_ref.at[t, pl.ds(0, n_high - 1)]
        wait_like(view, gb_send.at[t])
        wait_like(view, gb_recv.at[t])
        return jnp.sum(gb_ref[t], axis=0)

    def selectors():
        place = lax.broadcasted_iota(jnp.int32, (SUB, TILE), 1)
        owner, rank_of = place // rank_max, lax.rem(place, rank_max)

        def tile(i, carry):
            fc = jnp.zeros((SUB, TILE), jnp.int32)
            fr, keep = fc, fc
            for j in range(TILE // rank_max):
                b = i * (TILE // rank_max) + j
                fc = jnp.where(owner == j, fc_ref[b], fc)
                fr = jnp.where(owner == j, fr_ref[b], fr)
                keep = jnp.where(owner == j, rank_ref[b], keep)
            start = pl.multiple_of(i * TILE, TILE)
            sel_ref[0, :, pl.ds(start, TILE)] = jnp.where(rank_of < keep, fc, -1)
            sel_ref[1, :, pl.ds(start, TILE)] = fr
            return carry

        lax.fori_loop(0, far_tiles, tile, 0)

    def far_inner(t, late, i):
        first = lax.rem(row // half + late, n_row // half) * half
        q_half = ag_refs[t][pl.ds(first, half)].reshape(half * kcols, leaf)
        tile = slice(i * TILE, (i + 1) * TILE)
        y = jnp.dot(q_half, vt_t_ref[:, tile], preferred_element_type=jnp.float32)
        fc = jnp.concatenate([sel_ref[0, :, tile]] * (kcols // SUB), axis=0) - first
        inner = inner_ref[:, tile] if late else jnp.zeros((kcols, TILE), jnp.float32)
        for c in range(half):
            inner = jnp.where(fc == c, y[c * kcols : (c + 1) * kcols, :], inner)
        return inner

    def far_early(t):
        if half < n_row:
            for i in range(far_tiles):
                inner_ref[:, i * TILE : (i + 1) * TILE] = far_inner(t, 0, i)

    def operator(t):
        def far_tile(i):
            tile = slice(i * TILE, (i + 1) * TILE)
            inner = far_inner(t, int(half < n_row), i)
            fr = jnp.concatenate([sel_ref[1, :, tile]] * (kcols // SUB), axis=0)
            for r in range(n_col):
                lhs_ref[r * kcols : (r + 1) * kcols, tile] = jnp.where(
                    fr == r, inner, 0.0
                ).astype(jnp.bfloat16)

        def near_block(b, acc):
            z = jnp.dot(ag_refs[t][nc_ref[b]], near_ref[b], preferred_element_type=jnp.float32)
            r_of = nr_ref[b]
            return [
                a + z * jnp.where(r_of == r, 1.0, 0.0).astype(jnp.float32)
                for r, a in enumerate(acc)
            ]

        def far_chunk(g):
            chunk = slice(g * far_tiles // chunks * TILE, (g + 1) * far_tiles // chunks * TILE)
            far = jnp.dot(lhs_ref[:, chunk], ut_ref[chunk, :], preferred_element_type=jnp.float32)
            for r in range(n_col):
                piece = far[r * kcols : (r + 1) * kcols, :]
                part_ref[t, r] = part_ref[t, r] + piece if g else piece

        near = [jnp.zeros((kcols, leaf), jnp.float32)] * n_col
        done = 0
        n_early = n_near // 2
        for i in range(far_tiles):
            far_tile(i)
            for b in range(i * n_early // far_tiles, (i + 1) * n_early // far_tiles):
                near = near_block(b, near)
            if (done + 1) * far_tiles // chunks <= i + 1 - 1:
                far_chunk(done)
                done += 1
        while done < chunks:
            far_chunk(done)
            done += 1
        for b in range(n_early, n_near):
            near = near_block(b, near)
        for r in range(n_col):
            whole = part_ref[t, r] + near[r]
            part_ref[t, r] = whole
            out_ref[t, r] = whole.astype(jnp.bfloat16)

    lane = lax.broadcasted_iota(jnp.int32, (SUB, LANES), 1)
    lane_full = lax.broadcasted_iota(jnp.int32, (kcols, LANES), 1)
    sub_full = lax.broadcasted_iota(jnp.int32, (kcols, LANES), 0)

    def pack_gram(product):
        tiled = jnp.concatenate([product] * groups, axis=0)
        g = dot_nt(product, tiled, HIGH)
        rows = kcols // groups
        packed = jnp.zeros((rows, LANES), jnp.float32)
        for i in range(groups):
            packed = jnp.where(lane // kcols == i, g[i * rows : (i + 1) * rows, :], packed)
        return packed

    def solve(g):
        g = g / total_pts
        parts = []
        for i in range(groups):
            shift = (1 - i) * kcols % LANES
            parts.append(pltpu.roll(g, shift, 1) if shift else g)
        s = jnp.concatenate(parts, axis=0)
        work = jnp.where(lane_full < kcols, jnp.where(lane_full == sub_full, 1.0, 0.0), s)
        work = jnp.where(lane_full < 2 * kcols, work, 0.0)
        return factorize(work, kcols)


    loads[0].wait()
    pl.semaphore_wait(barrier, len(peers))
    gather_start(0)
    for copy in loads[1:4]:
        copy.wait()
    selectors()
    for i in range(n_parts):
        loads[7 + i].wait()
        for b in range(i * size, (i + 1) * size):
            near_ref[b] = near_ref[b].T
    loads[7 + n_parts].wait()
    for i in range(far_tiles):
        tile = slice(i * TILE, (i + 1) * TILE)
        vt_t_ref[:, tile] = vt_ref[tile, :].T
    for copy in (*loads[4:7], loads[8 + n_parts]):
        copy.wait()
    for t in range(ITERS):
        gather_wait(t, 0)
        far_early(t)
        if t > 0:
            gram_high_start(t - 1)
        gather_wait(t, 1)
        operator(t)
        scatter_start(t)
        if t > 0:
            rows = solve(gram_wait(t - 1))
        scatter_wait(t)
        total = part_ref[t, col]
        for d in range(1, n_col):
            total = total + rs_ref[t, d - 1].astype(jnp.float32)
        product = total * scale_ref[...]
        if t > 0:
            product = apply_inverse(rows, product)
        if t < ITERS - 1:
            ag_refs[t + 1][row] = product.astype(jnp.bfloat16)
            gather_start(t + 1)
            gram_low_start(t, pack_gram(product))
    prod_ref[...] = product
    rows_ref[...] = solve(gram_all(pack_gram(product)))


def on_device(
    q_start,
    row_scale,
    near_blocks,
    near_rows,
    near_cols,
    far_ut,
    far_vt,
    far_rank,
    far_rows,
    far_cols,
):
    leaf, kcols = q_start.shape
    n_row = lax.axis_size("row")
    n_col = lax.axis_size("col")
    n_dev = n_row * n_col
    pair = 2 if n_row % 2 == 0 else 1
    n_low, n_high = n_col * pair, n_row // pair
    n_near = near_blocks.shape[1]
    n_far, rank_max = far_ut.shape[1:3]
    near = near_blocks[0]
    ut = far_ut.reshape(n_far * rank_max, leaf)
    vt = far_vt.reshape(n_far * rank_max, leaf)
    vmem = pl.BlockSpec(memory_space=pltpu.VMEM)
    hbm = pl.BlockSpec(memory_space=pl.ANY)
    f32, bf16 = jnp.float32, jnp.bfloat16
    rows, product = pl.pallas_call(
        functools.partial(kernel, n_row, n_col, leaf * n_dev),
        name="subspace",
        out_shape=(
            pltpu.VMEM((kcols, LANES), f32),
            pltpu.VMEM((kcols, leaf), f32),
        ),
        in_specs=[hbm] * 10,
        out_specs=(vmem, vmem),
        scratch_shapes=[
            pltpu.VMEM((1, leaf), f32),
            pltpu.SMEM((n_far,), jnp.int32),
            pltpu.SMEM((n_far,), jnp.int32),
            pltpu.SMEM((n_far,), jnp.int32),
            pltpu.SMEM((n_near,), jnp.int32),
            pltpu.SMEM((n_near,), jnp.int32),
            pltpu.VMEM(near.shape, bf16),
            pltpu.VMEM(ut.shape, bf16),
            pltpu.VMEM(vt.shape, bf16),
            [pltpu.VMEM((n_row, kcols, leaf), bf16) for _ in range(ITERS)],
            pltpu.VMEM((2, SUB, n_far * rank_max), jnp.int32),
            pltpu.VMEM((kcols, n_far * rank_max), f32),
            pltpu.VMEM((n_col * kcols, n_far * rank_max), bf16),
            pltpu.VMEM((leaf, n_far * rank_max), bf16),
            pltpu.VMEM((ITERS, n_col, kcols, leaf), f32),
            pltpu.VMEM((ITERS, n_col, kcols, leaf), bf16),
            pltpu.VMEM((ITERS, n_col - 1, kcols, leaf), bf16),
            pltpu.VMEM((ITERS - 1, n_low, kcols * kcols // LANES, LANES), f32),
            pltpu.VMEM((ITERS - 1, n_high, kcols * kcols // LANES, LANES), f32),
            pltpu.VMEM((n_dev, kcols * kcols // LANES, LANES), f32),
            pltpu.SemaphoreType.DMA((13,)),
            pltpu.SemaphoreType.DMA((ITERS, 2)),
            pltpu.SemaphoreType.DMA((ITERS, 2)),
            pltpu.SemaphoreType.DMA((ITERS,)),
            pltpu.SemaphoreType.DMA((ITERS,)),
            pltpu.SemaphoreType.DMA((ITERS - 1,)),
            pltpu.SemaphoreType.DMA((ITERS - 1,)),
            pltpu.SemaphoreType.DMA((ITERS - 1,)),
            pltpu.SemaphoreType.DMA((ITERS - 1,)),
            pltpu.SemaphoreType.DMA((2,)),
        ],
        compiler_params=pltpu.CompilerParams(
            collective_id=0, has_side_effects=True, vmem_limit_bytes=56 * 1024 * 1024
        ),
    )(
        q_start.T,
        row_scale.reshape(1, leaf),
        far_rank[0, 0],
        far_rows[0, 0],
        far_cols[0, 0],
        near_rows[0, 0],
        near_cols[0, 0],
        near,
        ut,
        vt,
    )
    basis_t, factor = pl.pallas_call(
        finish,
        name="finish",
        out_shape=(
            jax.ShapeDtypeStruct((kcols, leaf), f32),
            jax.ShapeDtypeStruct((kcols, kcols), f32),
        ),
        in_specs=[vmem, vmem],
        out_specs=(vmem, vmem),
    )(*(pltpu.with_memory_space_constraint(x, pltpu.VMEM) for x in (rows, product)))
    return basis_t.T, factor


def solution(mesh):
    in_specs = (
        P(("row", "col"), None),
        P(("row", "col")),
        P("row", "col", None, None),
        P("row", "col", None),
        P("row", "col", None),
        P("row", "col", None, None),
        P("row", "col", None, None),
        P("row", "col", None),
        P("row", "col", None),
        P("row", "col", None),
    )
    out_specs = (P(("row", "col"), None), P())
    return jax.shard_map(
        on_device, mesh=mesh, in_specs=in_specs, out_specs=out_specs, check_vma=False
    )
```
